512 devices in a mesh: frow: 32 (over z_lo, y, core), fcol: 16 (over z_hi, x).
Axes of the slice: x: 4, y: 4, z: 16 (z_hi: 4, z_lo: 4; z = z_hi * 4 + z_lo), core: 2. Of those that a mesh axis runs over, the one named last changes fastest.
Arguments:
- model_image: bfloat16 [16384, 16384], P('frow', 'fcol'), may hold values from -6 to 6
- weight_grids: bfloat16 [8, 256, 256], replicated, may hold values from 0.19921875 to 2
- strip_offsets: int32 [2], replicated, may hold values from 0 to 63
- subgrid_offsets: int32 [2, 32], replicated, may hold values from 0 to 63
- grid_index: int32 [2, 32], replicated, may hold values from 0 to 7
Outputs:
- residual_update: float32 [16384, 16384], P('frow', 'fcol')
The draws below stay inside these ranges and needn't reach their ends.
Inputs may be any that keep to these rules, and one draw needn't show every extreme that they name: `strip_offsets`: two strips may coincide. `subgrid_offsets`: two subgrids of one strip may coincide.
All inputs are finite; a program needn't handle non-finite values.
Results may differ from the reference program's by a relative error of at most 0.03.
Values may be sent and summed in bfloat16 or wider, within the bound.
No kernel may reach another device: no remote copies, remote signals or barrier semaphores. Data moves between devices by JAX's collectives and lax.ppermute only.
A program may use at most 64 MiB of HBM per device.

```python
import math
import jax
import jax.numpy as jnp
from jax import lax

STRIP = 256
SUB = 256
STRIPS = 2
GRIDS = 8
IMAGE = 16384
SUBGRIDS = 32
N_FROW = 32


def touch_ends(values, stream_key, least, top_value):
    index_at = [jax.random.randint(jax.random.fold_in(stream_key, axis), (), 0, length) for axis, length in enumerate(values.shape)]
    widest = values.shape.index(max(values.shape))
    neighbour = index_at[:widest] + [(index_at[widest] + 1) % values.shape[widest]] + index_at[widest + 1:]
    return values.at[tuple(index_at)].set(least).at[tuple(neighbour)].set(top_value)


def block_levels(own_key, dims, cuts, low, top_value):
    factor_of = 1.0
    for axis_at, parts in cuts:
        steps = jax.random.uniform(jax.random.fold_in(jax.random.fold_in(own_key, 6), axis_at), (parts,), jnp.float32, low / len(cuts), top_value / len(cuts))
        factor_of = factor_of * jnp.repeat(jnp.exp(steps), dims[axis_at] // parts).reshape((-1,) + (1,) * (len(dims) - 1 - axis_at))
    return factor_of


def scatter_about(key, extent, scale, most, cuts=(), kind=jnp.bfloat16):
    loudness = block_levels(key, extent, cuts, -0.22, 0.18) if cuts else 1.0
    result = jax.random.normal(key, extent, jnp.float32) * scale * loudness
    return jnp.minimum(jnp.maximum(result, -most), most).astype(kind)


def setup_inputs(seed: int = 0) -> dict:
    keys = jax.random.split(jax.random.key(seed), 6)
    return {
        "model_image": scatter_about(keys[0], (IMAGE, IMAGE), 1.0, 6.0, ((0, 32), (1, 16))),
        "weight_grids": jnp.clip(jnp.exp(jax.random.uniform(keys[1], (GRIDS, STRIP, SUB), jnp.float32, math.log(0.19921875), math.log(2.0))), 0.19921875, 2.0).astype(jnp.bfloat16),
        "strip_offsets": jax.random.randint(keys[2], (STRIPS,), 0, IMAGE // STRIP).astype(jnp.int32),
        "subgrid_offsets": touch_ends(jax.random.randint(keys[3], (STRIPS, SUBGRIDS), 0, IMAGE // SUB), jax.random.fold_in(keys[3], 1), 0, (IMAGE // SUB) - 1).astype(jnp.int32),
        "grid_index": touch_ends(jax.random.randint(keys[4], (STRIPS, SUBGRIDS), 0, GRIDS), jax.random.fold_in(keys[4], 1), 0, GRIDS - 1).astype(jnp.int32),
    }


def phase_pair(leading, trailing, modulus, factor):
    turns = leading[:, None] * trailing[None, :] % modulus
    angle = turns.astype(jnp.float32) * (2.0 * math.pi / modulus)
    return (jnp.cos(angle) * factor, jnp.sin(angle) * factor)

def modulate(strip_real, strip_imag, cos_shift, sin_shift):
    real_part = strip_real[None] * cos_shift[:, None, :] + strip_imag[None] * sin_shift[:, None, :]
    imag_part = strip_imag[None] * cos_shift[:, None, :] - strip_real[None] * sin_shift[:, None, :]
    return jnp.concatenate([real_part, imag_part], axis=2).astype(jnp.bfloat16)

def demodulate(spectra, cos_shift, sin_shift, width):
    real_in = spectra[:, :, :width]
    imag_in = spectra[:, :, width:]
    real_part = lax.optimization_barrier(jnp.sum(real_in * cos_shift[:, None, :] - imag_in * sin_shift[:, None, :], axis=0))
    imag_part = lax.optimization_barrier(jnp.sum(imag_in * cos_shift[:, None, :] + real_in * sin_shift[:, None, :], axis=0))
    return jnp.concatenate([real_part, imag_part], axis=1)

def forward_table(pixels, sub_width, modulus, factor):
    spaced = jnp.arange(sub_width, dtype=jnp.int32) * (modulus // sub_width)
    cosine, sine = phase_pair(pixels, spaced, modulus, factor)
    upper = jnp.concatenate([cosine, -sine], axis=1)
    lower = jnp.concatenate([sine, cosine], axis=1)
    return jnp.concatenate([upper, lower], axis=0).astype(jnp.bfloat16)

def backward_table(pixels, sub_width, modulus, factor):
    spaced = jnp.arange(sub_width, dtype=jnp.int32) * (modulus // sub_width)
    cosine, sine = phase_pair(spaced, pixels, modulus, factor)
    upper = jnp.concatenate([cosine, sine], axis=1)
    lower = jnp.concatenate([-sine, cosine], axis=1)
    return jnp.concatenate([upper, lower], axis=0).astype(jnp.bfloat16)

def reference(model_image, weight_grids, strip_offsets, subgrid_offsets, grid_index):
    rows_local = IMAGE // N_FROW
    uv_rows = STRIPS * STRIP
    forward_scale = 1.0 / math.sqrt(IMAGE)
    column_scale = 1.0 / math.sqrt(SUBGRIDS * SUB)
    row_scale = 1.0 / math.sqrt(uv_rows)
    row_spacing = IMAGE // STRIP
    frequencies = (strip_offsets[:, None] + jnp.arange(STRIP, dtype=jnp.int32)[None, :] * row_spacing).reshape(uv_rows)

    def strip_block(totals, group):
        first_row = group * rows_local
        pixel_rows = first_row + jnp.arange(rows_local, dtype=jnp.int32)
        cosine, sine = phase_pair(frequencies, pixel_rows, IMAGE, forward_scale)
        phases = jnp.concatenate([cosine, sine], axis=0).astype(jnp.bfloat16)
        row_block = lax.dynamic_slice_in_dim(model_image, first_row, rows_local, 0)
        stacked = jnp.dot(phases, row_block, preferred_element_type=jnp.float32)
        joined = jnp.concatenate([stacked[:uv_rows], -stacked[uv_rows:]], axis=1)
        rounded = lax.optimization_barrier(joined.astype(jnp.bfloat16))
        return (totals + rounded.astype(jnp.float32), None)
    start_totals = jnp.zeros((uv_rows, 2 * IMAGE), jnp.float32)
    totals, _ = lax.scan(strip_block, start_totals, jnp.arange(N_FROW, dtype=jnp.int32))
    strip = totals.astype(jnp.bfloat16)
    pixel_cols = jnp.arange(IMAGE, dtype=jnp.int32)
    ahead = forward_table(pixel_cols, SUB, IMAGE, forward_scale)
    behind = backward_table(pixel_cols, SUB, IMAGE, column_scale)
    images = []
    for strip_number in range(STRIPS):
        rows_here = strip[strip_number * STRIP:(strip_number + 1) * STRIP]
        strip_real = rows_here[:, :IMAGE]
        strip_imag = rows_here[:, IMAGE:]

        def one_subgrid(running, item):
            shift_value, chosen = item
            cos_shift, sin_shift = phase_pair(shift_value[None], pixel_cols, IMAGE, 1.0)
            modulated = modulate(strip_real, strip_imag, cos_shift, sin_shift)[0]
            spectra = jnp.dot(modulated, ahead, preferred_element_type=jnp.float32)
            grid = lax.dynamic_index_in_dim(weight_grids, chosen, 0, keepdims=False).astype(jnp.float32)
            weighted = (spectra * jnp.concatenate([grid, grid], axis=1)).astype(jnp.bfloat16)
            returned = jnp.dot(weighted, behind, preferred_element_type=jnp.float32)[None]
            return (running + demodulate(returned, cos_shift, sin_shift, IMAGE), None)
        start_sum = jnp.zeros((STRIP, 2 * IMAGE), jnp.float32)
        merged, _ = lax.scan(one_subgrid, start_sum, (subgrid_offsets[strip_number], grid_index[strip_number]))
        images.append(merged.astype(jnp.bfloat16))
    strip_image = jnp.concatenate(images, axis=0)
    all_rows = jnp.arange(IMAGE, dtype=jnp.int32)
    cosine, sine = phase_pair(all_rows, frequencies, IMAGE, row_scale)
    phases = jnp.concatenate([cosine, -sine], axis=1).astype(jnp.bfloat16)
    stacked = jnp.concatenate([strip_image[:, :IMAGE], strip_image[:, IMAGE:]], axis=0)
    return jnp.dot(phases, stacked, preferred_element_type=jnp.float32)
```

```python
import math

import jax
import jax.numpy as jnp
import numpy as np
from jax import lax
from jax.sharding import Mesh
from jax.sharding import PartitionSpec as P

F32 = jnp.float32
BF16 = jnp.bfloat16
STRIP = 256
SUB = 256
AXES = ("zl", "y", "core", "zh", "x")
NEAR = ("zl", "y", "x")


def turn(numerator, denominator):
    angle = (numerator % denominator).astype(F32) * (2.0 * math.pi / denominator)
    return jnp.cos(angle), jnp.sin(angle)


def tables(quads, blocks, sub_cols, uv_cols):
    r = np.arange(STRIP).reshape(quads, 1, -1, 1, 1)
    p = np.arange(2).reshape(1, 2, 1, 1, 1)
    q = np.arange(2).reshape(1, 1, 1, 2, 1)
    b = np.arange(STRIP).reshape(1, 1, 1, 1, -1)
    phase = 2.0 * np.pi * ((r * b) % STRIP) / STRIP + (p - q) * (np.pi / 2)
    phase = phase.reshape(2 * STRIP, 2 * STRIP)
    rows = (np.cos(phase), -np.sin(phase))
    d = np.arange(SUB)
    phase = 2.0 * np.pi * (np.outer(d, d) % SUB) / SUB
    cos, sin = np.cos(phase), np.sin(phase)
    cols = np.block([[cos, -sin], [sin, cos]])
    u = np.arange(uv_cols).reshape(1, -1, 1, 1, 1)
    p = np.arange(2).reshape(2, 1, 1, 1, 1)
    c = blocks.reshape(1, 1, -1, 1, 1)
    q = np.arange(2).reshape(1, 1, 1, 2, 1)
    phase = 2.0 * np.pi * ((u * c) % uv_cols) / uv_cols + (p - q) * (np.pi / 2)
    phase = np.broadcast_to(np.cos(phase), (2, uv_cols, blocks.size, 2, sub_cols))
    return rows, cols, phase.reshape(2, uv_cols, -1)


def body(model_image, weight_grids, strip_offsets, subgrid_offsets, grid_index):
    rows_local, facet_width = model_image.shape
    ny, nx, nzl, nzh = (lax.axis_size(a) for a in ("y", "x", "zl", "zh"))
    ncore = lax.axis_size("core")
    zl, y, core, zh, x = (lax.axis_index(a) for a in AXES)
    width = facet_width // ny
    modulus = facet_width * nx * nzh
    uv_cols = modulus // SUB
    periods = rows_local // STRIP
    quads = nzl * ny * nx
    rows_each = STRIP // quads
    count = subgrid_offsets.shape[1]
    strips = strip_offsets.shape[0]

    order = np.arange(uv_cols).reshape(nzh, nx, ny).transpose(0, 2, 1).reshape(-1)
    (rows_cos, rows_sin), cols_table, block_table = tables(quads, order, rows_each, uv_cols)

    own, other = core, 1 - core
    offset_own = lax.dynamic_index_in_dim(strip_offsets, own, 0, keepdims=False)
    offset_other = lax.dynamic_index_in_dim(strip_offsets, other, 0, keepdims=False)
    span = (zl * ny + jnp.arange(ny, dtype=jnp.int32)) * ncore + core
    span = span[:, None] * periods + jnp.arange(periods, dtype=jnp.int32)
    own_cos, own_sin = turn(offset_own * span, uv_cols)
    other_cos, other_sin = turn(offset_other * span, uv_cols)

    cos_b, sin_b = turn(offset_own * jnp.arange(STRIP, dtype=jnp.int32), modulus)
    cos_b = jnp.concatenate([cos_b, cos_b])[None]
    sin_b = jnp.concatenate([sin_b, sin_b])[None]
    row_phases = (
        jnp.asarray(rows_cos, BF16).astype(F32) * cos_b
        + jnp.asarray(rows_sin, BF16).astype(F32) * sin_b
    ).astype(BF16)

    gathered = lax.all_to_all(model_image, "y", 1, 0, tiled=True)
    pixels = gathered.reshape(ny, periods, STRIP, width).astype(F32)

    def fold(cos, sin):
        real = jnp.sum(pixels * cos[:, :, None, None], axis=(0, 1))
        imag = -jnp.sum(pixels * sin[:, :, None, None], axis=(0, 1))
        return jnp.concatenate([real, imag], axis=0)

    swap = [(0, 1), (1, 0)]
    received = lax.ppermute(fold(other_cos, other_sin).astype(BF16), "core", swap)
    folded = (fold(own_cos, own_sin) + received.astype(F32)).astype(BF16)
    partial = jnp.dot(row_phases, folded, preferred_element_type=F32).astype(BF16)

    parts = lax.all_to_all(partial.reshape(quads, 2 * rows_each, width), NEAR, 0, 0, tiled=True)
    parts = parts.reshape(nzl, ny * nx, 2 * rows_each, width).astype(F32)
    strip = jnp.sum(parts, axis=0).astype(BF16).reshape(ny * nx * 2 * rows_each, width)
    whole = lax.all_gather(strip, "zh", axis=0, tiled=True)

    quad = (zl * ny + y) * nx + x
    shifts = lax.dynamic_index_in_dim(subgrid_offsets, own, 0, keepdims=False)
    chosen = lax.dynamic_index_in_dim(grid_index, own, 0, keepdims=False)
    lines = rows_each * count
    line_shift = jnp.tile(shifts, rows_each)
    line_row = jnp.repeat(jnp.arange(rows_each, dtype=jnp.int32), count)
    pick = (line_shift[:, None] == jnp.arange(uv_cols, dtype=jnp.int32)[None]).astype(BF16)
    table_row = jnp.arange(2 * uv_cols * rows_each, dtype=jnp.int32) % rows_each
    same = line_row[:, None] == table_row[None]
    spread = [
        jnp.where(same, jnp.dot(pick, jnp.asarray(block_table[part], BF16), preferred_element_type=F32), 0.0)
        for part in range(2)
    ]
    spread = jnp.concatenate(spread, axis=0).astype(BF16)
    cos_d, sin_d = turn(shifts[:, None] * jnp.arange(SUB, dtype=jnp.int32)[None], modulus)
    cos_d = jnp.tile(cos_d, (rows_each, 1))
    sin_d = jnp.tile(sin_d, (rows_each, 1))
    fourier = jnp.asarray(cols_table, BF16)

    mixed = jnp.dot(spread, whole, preferred_element_type=F32)
    real, imag = mixed[:lines], mixed[lines:]
    turned = jnp.concatenate(
        [real * cos_d + imag * sin_d, imag * cos_d - real * sin_d], axis=1
    ).astype(BF16)
    spectra = jnp.dot(turned, fourier, preferred_element_type=F32)
    grid_rows = lax.dynamic_slice_in_dim(weight_grids, quad * rows_each, rows_each, 1)
    grids = grid_rows.shape[0]
    line_grid = jnp.tile(chosen, rows_each)[:, None] * rows_each + line_row[:, None]
    select = (line_grid == jnp.arange(grids * rows_each, dtype=jnp.int32)[None]).astype(BF16)
    weights = jnp.dot(select, grid_rows.reshape(grids * rows_each, SUB), preferred_element_type=F32)
    weighted = (spectra * jnp.concatenate([weights, weights], axis=1)).astype(BF16)

    returned = lax.dot_general(
        weighted, fourier, (((1,), (1,)), ((), ())), preferred_element_type=F32
    )
    real, imag = returned[:, :SUB], returned[:, SUB:]
    turned = jnp.concatenate(
        [real * cos_d - imag * sin_d, imag * cos_d + real * sin_d], axis=0
    ).astype(BF16)
    held = strip.shape[0]
    mine = lax.dynamic_slice_in_dim(spread, zh * held, held, 1)
    back = lax.dot_general(mine, turned, (((0,), (0,)), ((), ())), preferred_element_type=F32)
    back = back.astype(BF16).reshape(ny * nx, 2 * rows_each, width)
    back = jnp.tile(back, (nzl, 1, 1))
    image = lax.all_to_all(back, NEAR, 0, 0, tiled=True).reshape(2 * STRIP, width)

    scale = 1.0 / (modulus * math.sqrt(count * SUB) * math.sqrt(strips * STRIP))
    expanded = lax.dot_general(
        row_phases, image, (((0,), (0,)), ((), ())), preferred_element_type=F32
    )
    expanded = (expanded * scale).astype(BF16)
    received = lax.ppermute(expanded, "core", swap)

    def unfold(value, cos, sin):
        value = value.astype(F32)[None, None]
        real, imag = value[:, :, :STRIP], value[:, :, STRIP:]
        return real * cos[:, :, None, None] - imag * sin[:, :, None, None]

    update = unfold(expanded, own_cos, own_sin) + unfold(received, other_cos, other_sin)
    update = update.astype(BF16).reshape(ny * rows_local, width)
    return lax.all_to_all(update, "y", 0, 1, tiled=True).astype(F32)


def solution(mesh):
    shape = {"zl": 4, "y": 4, "core": 2, "zh": 4, "x": 4}
    finer = Mesh(mesh.devices.reshape(tuple(shape.values())), tuple(shape))
    rows, cols = ("zl", "y", "core"), ("zh", "x")
    return jax.shard_map(
        body,
        mesh=finer,
        in_specs=(P(rows, cols), P(), P(), P(), P()),
        out_specs=P(rows, cols),
        check_vma=False,
    )
```

```python
import functools
import math

import jax
import jax.numpy as jnp
import ml_dtypes
import numpy as np
from jax import lax
from jax.experimental import pallas as pl
from jax.experimental.pallas import tpu as pltpu
from jax.sharding import Mesh
from jax.sharding import PartitionSpec as P

F32 = jnp.float32
BF16 = jnp.bfloat16
I32 = jnp.int32
STRIP = 256
SUB = 256
GRID = {"zl": 4, "y": 4, "core": 2, "zh": 4, "x": 4}
VMEM = pltpu.VMEM
SMEM = pltpu.SMEM
MIB = 1 << 20


def grant(mib):
    return pltpu.CompilerParams(vmem_limit_bytes=mib * MIB)


def turn(numerator, denominator):
    angle = (numerator % denominator).astype(F32) * (2.0 * math.pi / denominator)
    return jnp.cos(angle), jnp.sin(angle)


def fixed(values):
    return jnp.asarray(np.asarray(values, dtype=ml_dtypes.bfloat16))


def row_table(rows_each):
    r = np.arange(STRIP).reshape(-1, 1, rows_each, 1, 1)
    p = np.arange(2).reshape(1, 2, 1, 1, 1)
    q = np.arange(2).reshape(1, 1, 1, 2, 1)
    b = np.arange(STRIP).reshape(1, 1, 1, 1, -1)
    phase = 2.0 * np.pi * ((r * b) % STRIP) / STRIP + (p - q) * (np.pi / 2)
    phase = phase.reshape(2 * STRIP, 2 * STRIP)
    return fixed(np.cos(phase))


def column_table():
    d = np.arange(SUB)
    phase = 2.0 * np.pi * (np.outer(d, d) % SUB) / SUB
    cos, sin = np.cos(phase), np.sin(phase)
    return fixed(np.block([[cos, -sin], [sin, cos]]))


def block_tables(order, uv_cols, rows_each):
    u = np.arange(uv_cols).reshape(1, -1, 1, 1, 1, 1)
    p = np.arange(2).reshape(2, 1, 1, 1, 1, 1)
    c = order.reshape(1, 1, -1, 1, 1, 1)
    q = np.arange(2).reshape(1, 1, 1, 2, 1, 1)
    phase = 2.0 * np.pi * ((u * c) % uv_cols) / uv_cols + (p - q) * (np.pi / 2)
    table = np.broadcast_to(np.cos(phase), (2, uv_cols, order.size, 2, rows_each, 1))
    return fixed(table.reshape(2, uv_cols, -1))


def coefficients(strip, periods, uv_cols, offset_ref):
    zl, y, core = (lax.axis_index(a) for a in ("zl", "y", "core"))
    first = ((zl * GRID["y"] + y) * GRID["core"] + core) * periods
    pairs = []
    for a in range(periods):
        place = (offset_ref[strip] * (first + a)) & (uv_cols - 1)
        cos, sin = F32(1.0), F32(0.0)
        for digit in range(uv_cols.bit_length() - 1):
            angle = 2.0 * math.pi * (1 << digit) / uv_cols
            by_cos, by_sin = round(math.cos(angle), 15), round(math.sin(angle), 15)
            on = ((place >> digit) & 1) == 1
            cos, sin = (
                jnp.where(on, cos * by_cos - sin * by_sin, cos),
                jnp.where(on, sin * by_cos + cos * by_sin, sin),
            )
        pairs.append((cos, sin))
    return pairs


def fold_block(pairs, image_ref, out_ref, first, rows):
    step, width = 16, 512
    for at in range(first, first + rows, step):
        for lane in range(0, image_ref.shape[1], width):
            lanes = slice(lane, lane + width)
            real = imag = 0.0
            for a, (cos, sin) in enumerate(pairs):
                pixels = image_ref[a * STRIP + at : a * STRIP + at + step, lanes].astype(F32)
                real = real + pixels * cos
                imag = imag - pixels * sin
            out_ref[at : at + step, lanes] = real.astype(BF16)
            out_ref[STRIP + at : STRIP + at + step, lanes] = imag.astype(BF16)


def fold_other_kernel(uv_cols, offset_hbm, image_hbm, out_ref, image_ref, offset_ref, sems):
    periods = image_ref.shape[0] // STRIP
    pieces = 4
    rows = STRIP // pieces
    ahead = pltpu.make_async_copy(offset_hbm, offset_ref, sems.at[0])
    ahead.start()
    copies = []
    for n in range(pieces):
        for a in range(periods):
            at = pl.ds(a * STRIP + n * rows, rows)
            copies.append(
                pltpu.make_async_copy(image_hbm.at[at], image_ref.at[at], sems.at[1 + len(copies)])
            )
            copies[-1].start()
    ahead.wait()
    pairs = coefficients(1 - lax.axis_index("core"), periods, uv_cols, offset_ref)
    for n in range(pieces):
        for a in range(periods):
            copies[n * periods + a].wait()
        fold_block(pairs, image_ref, out_ref, n * rows, rows)


def fold_own_kernel(uv_cols, offset_ref, image_ref, out_ref):
    pairs = coefficients(lax.axis_index("core"), image_ref.shape[0] // STRIP, uv_cols, offset_ref)
    fold_block(pairs, image_ref, out_ref, 0, STRIP)


def phase_kernel(table_ref, cos_ref, sin_ref, phases_ref):
    core = pl.ds(lax.axis_index("core"), 1)
    cos, sin = cos_ref[core, :], sin_ref[core, :]
    left = table_ref[:, :STRIP].astype(F32)
    right = table_ref[:, STRIP:].astype(F32)
    phases_ref[:, :STRIP] = (left * cos - right * sin).astype(BF16)
    phases_ref[:, STRIP:] = (right * cos + left * sin).astype(BF16)


def row_kernel(phases_ref, own_ref, other_ref, out_ref):
    step = 256
    for lane in range(0, own_ref.shape[1], step):
        lanes = slice(lane, lane + step)
        total = (own_ref[:, lanes].astype(F32) + other_ref[:, lanes].astype(F32)).astype(BF16)
        out_ref[:, lanes] = jnp.dot(phases_ref[...], total, preferred_element_type=F32).astype(BF16)


def sum_kernel(parts_ref, out_ref):
    step, width = 16, 512
    for at in range(0, out_ref.shape[0], step):
        for lane in range(0, out_ref.shape[1], width):
            here = (slice(at, at + step), slice(lane, lane + width))
            total = parts_ref[(0, *here)].astype(F32)
            for n in range(1, parts_ref.shape[0]):
                total = total + parts_ref[(n, *here)].astype(F32)
            out_ref[here] = total.astype(BF16)


def tables_kernel(rows_each, shift_ref, chosen_ref, grid_ref, table_ref, spread_ref, weight_ref):
    count = shift_ref.shape[1]
    core = pl.ds(lax.axis_index("core"), 1)
    uv_cols, columns = table_ref.shape[1:]
    over_rows = (((0,), (0,)), ((), ()))

    def one_hot(condition):
        return jnp.where(condition, 1.0, 0.0).astype(BF16)

    pick = one_hot(lax.broadcasted_iota(I32, (uv_cols, count), 0) == shift_ref[core, :])
    row = lax.broadcasted_iota(I32, (count, columns), 1) & (rows_each - 1)
    for part in range(2):
        lines = lax.dot_general(pick, table_ref[part], over_rows, preferred_element_type=F32)
        for i in range(rows_each):
            at = (part * rows_each + i) * count
            spread_ref[at : at + count, :] = jnp.where(row == i, lines, 0.0).astype(BF16)

    tile = 16
    first = rows_each * ((lax.axis_index("y") * GRID["zl"] + lax.axis_index("zl")) * GRID["x"] + lax.axis_index("x"))
    base = pl.multiple_of((first // tile) * tile, tile)
    grids = grid_ref.shape[0]
    rows = jnp.concatenate([grid_ref[g, pl.ds(base, tile), :] for g in range(grids)], axis=0)
    line = lax.broadcasted_iota(I32, (grids * tile, count), 0)
    chosen = chosen_ref[core, :] * tile + (first - base)
    for i in range(rows_each):
        pick = one_hot(line == chosen + i)
        weight_ref[i * count : (i + 1) * count, :] = lax.dot_general(
            pick, rows, over_rows, preferred_element_type=F32
        )


def middle_kernel(lines, spread_ref, cos_ref, sin_ref, weight_ref, fourier_ref, strip_ref, out_ref):
    nzh, nzl = GRID["zh"], GRID["zl"]
    held = strip_ref.shape[0] // nzh
    blocks = strip_ref.shape[1] // SUB
    pieces = [
        strip_ref[z * held : (z + 1) * held, c * SUB : (c + 1) * SUB]
        for z in range(nzh)
        for c in range(blocks)
    ]
    whole = jnp.concatenate(pieces, axis=0)
    mixed = jnp.dot(spread_ref[...], whole, preferred_element_type=F32)
    repeat = lines // cos_ref.shape[0]
    cos = jnp.concatenate([cos_ref[...]] * repeat, axis=0)
    sin = jnp.concatenate([sin_ref[...]] * repeat, axis=0)
    real, imag = mixed[:lines], mixed[lines:]
    turned = jnp.concatenate([real * cos + imag * sin, imag * cos - real * sin], axis=1)
    spectra = jnp.dot(turned.astype(BF16), fourier_ref[...], preferred_element_type=F32)
    weight = weight_ref[...]
    weighted = jnp.concatenate([spectra[:, :SUB] * weight, -spectra[:, SUB:] * weight], axis=1)
    returned = jnp.dot(weighted.astype(BF16), fourier_ref[...], preferred_element_type=F32)
    real, imag = returned[:, :SUB], -returned[:, SUB:]
    turned = jnp.concatenate([real * cos - imag * sin, imag * cos + real * sin], axis=0)
    inside = held * blocks
    mine = spread_ref[:, pl.ds(pl.multiple_of(lax.axis_index("zh") * inside, inside), inside)]
    back = lax.dot_general(
        mine, turned.astype(BF16), (((0,), (0,)), ((), ())), preferred_element_type=F32
    ).astype(BF16)
    for z in range(nzl):
        for c in range(blocks):
            out_ref[z * held : (z + 1) * held, c * SUB : (c + 1) * SUB] = back[c * held : (c + 1) * held]


def unfold_kernel(uv_cols, offset_ref, own_ref, other_ref, out_hbm, held_ref, sems):
    core = lax.axis_index("core")
    periods, rows, lanes_all = held_ref.shape
    own = coefficients(core, periods, uv_cols, offset_ref)
    other = coefficients(1 - core, periods, uv_cols, offset_ref)
    step, width = 16, 256
    piece = 32
    copies = []
    for n in range(0, rows, step):
        for lane in range(0, lanes_all, width):
            lanes = slice(lane, lane + width)
            parts = [
                ref[part * STRIP + n : part * STRIP + n + step, lanes].astype(F32)
                for ref in (own_ref, other_ref)
                for part in range(2)
            ]
            for a in range(periods):
                held_ref[a, n : n + step, lanes] = (
                    parts[0] * own[a][0]
                    - parts[1] * own[a][1]
                    + parts[2] * other[a][0]
                    - parts[3] * other[a][1]
                )
        if (n + step) % piece == 0:
            at = pl.ds(n + step - piece, piece)
            for a in range(periods):
                copies.append(
                    pltpu.make_async_copy(held_ref.at[a, at], out_hbm.at[a, at], sems.at[len(copies)])
                )
                copies[-1].start()
    for copy in copies:
        copy.wait()


def body(model_image, weight_grids, strip_offsets, subgrid_offsets, grid_index):
    rows_local, facet_width = model_image.shape
    ny, nx, nzl, nzh = (GRID[a] for a in ("y", "x", "zl", "zh"))
    core = lax.axis_index("core")
    modulus = facet_width * nx * nzh
    uv_cols = modulus // SUB
    periods = rows_local // STRIP
    rows_each = STRIP // (nzl * ny * nx)
    count = subgrid_offsets.shape[1]
    strips = strip_offsets.shape[0]
    blocks = facet_width // SUB
    vmem = pl.BlockSpec(memory_space=VMEM)
    smem = pl.BlockSpec(memory_space=SMEM)
    half = jax.ShapeDtypeStruct((2 * STRIP, facet_width), BF16)

    hbm = pl.BlockSpec(memory_space=pltpu.HBM)

    other = pl.pallas_call(
        functools.partial(fold_other_kernel, uv_cols),
        out_shape=half,
        in_specs=[hbm, hbm],
        out_specs=vmem,
        scratch_shapes=[
            VMEM(model_image.shape, BF16),
            SMEM(strip_offsets.shape, I32),
            pltpu.SemaphoreType.DMA((16,)),
        ],
        compiler_params=grant(8),
        name="fold_other",
    )(*(pltpu.with_memory_space_constraint(a, pltpu.HBM) for a in (strip_offsets, model_image)))
    swap = [(0, 1), (1, 0)]
    received = lax.ppermute(other, "core", swap)
    folded = pl.pallas_call(
        functools.partial(fold_own_kernel, uv_cols),
        out_shape=half,
        in_specs=[smem, vmem],
        out_specs=vmem,
        cost_estimate=pl.CostEstimate(flops=4 * MIB, bytes_accessed=2 * MIB, transcendentals=0),
        compiler_params=grant(8),
        name="fold_own",
    )(strip_offsets, model_image)

    cos_b, sin_b = turn(
        strip_offsets[:, None] * jnp.arange(STRIP, dtype=I32)[None], modulus
    )
    phases = pl.pallas_call(
        phase_kernel,
        out_shape=jax.ShapeDtypeStruct((2 * STRIP, 2 * STRIP), BF16),
        in_specs=[vmem] * 3,
        out_specs=vmem,
        cost_estimate=pl.CostEstimate(flops=MIB, bytes_accessed=2 * MIB, transcendentals=0),
        compiler_params=grant(8),
        name="phases",
    )(row_table(rows_each), cos_b, sin_b)
    partial = pl.pallas_call(
        row_kernel,
        out_shape=half,
        in_specs=[vmem] * 3,
        out_specs=vmem,
        compiler_params=grant(8),
        name="row_transform",
    )(phases, folded, received)

    lines = rows_each * count
    order = np.arange(uv_cols).reshape(nzh, nx, blocks).transpose(0, 2, 1).reshape(-1)
    table = block_tables(order, uv_cols, rows_each)
    spread, weights = pl.pallas_call(
        functools.partial(tables_kernel, rows_each),
        out_shape=(
            jax.ShapeDtypeStruct((2 * lines, table.shape[2]), BF16),
            jax.ShapeDtypeStruct((lines, SUB), F32),
        ),
        in_specs=[vmem] * 4,
        out_specs=(vmem, vmem),
        cost_estimate=pl.CostEstimate(flops=8 * MIB, bytes_accessed=MIB // 2, transcendentals=0),
        compiler_params=grant(4),
        name="tables",
    )(subgrid_offsets, grid_index, weight_grids, table)
    shifts = lax.dynamic_index_in_dim(subgrid_offsets, core, 0, keepdims=False)
    cos_d, sin_d = turn(shifts[:, None] * jnp.arange(SUB, dtype=I32)[None], modulus)
    fourier = column_table()
    partial, spread, cos_d, sin_d, weights, fourier = lax.optimization_barrier(
        (partial, spread, cos_d, sin_d, weights, fourier)
    )
    parts = lax.all_to_all(partial.reshape(ny, -1, facet_width), "y", 0, 0, tiled=True)
    share = pl.pallas_call(
        sum_kernel,
        out_shape=jax.ShapeDtypeStruct(parts.shape[1:], BF16),
        in_specs=[vmem],
        out_specs=vmem,
        compiler_params=grant(4),
        name="row_sum",
    )(parts)
    parts = lax.all_to_all(
        share.reshape(nzl * nx, 2 * rows_each, facet_width), ("zl", "x"), 0, 0, tiled=True
    )
    parts = parts.reshape(nzl, nx * 2 * rows_each, facet_width)
    strip = jnp.sum(parts.astype(F32), axis=0).astype(BF16)
    whole = lax.all_gather(strip, "zh", axis=0, tiled=True)

    back = pl.pallas_call(
        functools.partial(middle_kernel, lines),
        out_shape=jax.ShapeDtypeStruct((nzl * nx * 2 * rows_each, facet_width), BF16),
        in_specs=[vmem] * 6,
        out_specs=vmem,
        compiler_params=grant(16),
        name="subgrids",
    )(spread, cos_d, sin_d, weights, fourier, whole)

    back = back.reshape(nzl * nx, 2 * rows_each, facet_width)
    back = lax.all_to_all(back, ("zl", "x"), 0, 0, tiled=True).reshape(1, -1, facet_width)
    back = jnp.broadcast_to(back, (ny, *back.shape[1:]))
    image = lax.all_to_all(back, "y", 0, 0, tiled=True).reshape(2 * STRIP, facet_width)

    scale = 1.0 / (modulus * math.sqrt(count * SUB) * math.sqrt(strips * STRIP))
    expanded = lax.dot_general(
        phases, image, (((0,), (0,)), ((), ())), preferred_element_type=F32
    )
    expanded = (expanded * scale).astype(BF16)
    received = lax.ppermute(expanded, "core", swap)

    shape = (periods, STRIP, facet_width)
    update = pl.pallas_call(
        functools.partial(unfold_kernel, uv_cols),
        out_shape=jax.ShapeDtypeStruct(shape, F32),
        in_specs=[smem, vmem, vmem],
        out_specs=hbm,
        scratch_shapes=[VMEM(shape, F32), pltpu.SemaphoreType.DMA((16,))],
        compiler_params=grant(8),
        name="unfold",
    )(strip_offsets, expanded, received)
    return update.reshape(rows_local, facet_width)


def solution(mesh):
    finer = Mesh(mesh.devices.reshape(tuple(GRID.values())), tuple(GRID))
    rows, cols = ("zl", "y", "core"), ("zh", "x")
    return jax.shard_map(
        body,
        mesh=finer,
        in_specs=(P(rows, cols), P(), P(), P(), P()),
        out_specs=P(rows, cols),
        check_vma=False,
    )
```

```python
import functools
import math

import jax
import jax.numpy as jnp
import ml_dtypes
import numpy as np
from jax import lax
from jax.experimental import pallas as pl
from jax.experimental.pallas import tpu as pltpu
from jax.sharding import Mesh
from jax.sharding import PartitionSpec as P

F32 = jnp.float32
BF16 = jnp.bfloat16
I32 = jnp.int32
STRIP = 256
SUB = 256
GRID = {"zl": 4, "y": 4, "core": 2, "zh": 4, "x": 4}
VMEM = pltpu.VMEM
SMEM = pltpu.SMEM
MIB = 1 << 20


def grant(mib):
    return pltpu.CompilerParams(vmem_limit_bytes=mib * MIB)


def turn(numerator, denominator):
    angle = (numerator % denominator).astype(F32) * (2.0 * math.pi / denominator)
    return jnp.cos(angle), jnp.sin(angle)


def fixed(values):
    return jnp.asarray(np.asarray(values, dtype=ml_dtypes.bfloat16))


def row_table(rows_each):
    r = np.arange(STRIP).reshape(-1, 1, rows_each, 1, 1)
    p = np.arange(2).reshape(1, 2, 1, 1, 1)
    q = np.arange(2).reshape(1, 1, 1, 2, 1)
    b = np.arange(STRIP).reshape(1, 1, 1, 1, -1)
    phase = 2.0 * np.pi * ((r * b) % STRIP) / STRIP + (p - q) * (np.pi / 2)
    return fixed(np.cos(phase.reshape(2 * STRIP, 2 * STRIP)))


def return_table(rows_each):
    b = np.arange(STRIP).reshape(-1, 1, 1, 1)
    r = np.arange(STRIP).reshape(1, -1, 1, rows_each)
    p = np.arange(2).reshape(1, 1, 2, 1)
    phase = (2.0 * np.pi * ((r * b) % STRIP) / STRIP + p * (np.pi / 2)).reshape(STRIP, 2 * STRIP)
    return fixed(np.concatenate([np.cos(phase), -np.sin(phase)], axis=0))


def column_table():
    d = np.arange(SUB)
    phase = 2.0 * np.pi * (np.outer(d, d) % SUB) / SUB
    cos, sin = np.cos(phase), np.sin(phase)
    return fixed(np.block([[cos, -sin], [sin, cos]]))


def block_tables(order, uv_cols, rows_each):
    u = np.arange(uv_cols).reshape(1, -1, 1, 1, 1, 1)
    p = np.arange(2).reshape(2, 1, 1, 1, 1, 1)
    c = order.reshape(1, 1, -1, 1, 1, 1)
    q = np.arange(2).reshape(1, 1, 1, 2, 1, 1)
    phase = 2.0 * np.pi * ((u * c) % uv_cols) / uv_cols + (p - q) * (np.pi / 2)
    table = np.broadcast_to(np.cos(phase), (2, uv_cols, order.size, 2, rows_each, 1))
    return fixed(table.reshape(2, uv_cols, -1))


def coefficients(strip, rows_of, periods, uv_cols, offset_ref):
    zl, y = (lax.axis_index(a) for a in ("zl", "y"))
    first = ((zl * GRID["y"] + y) * GRID["core"] + rows_of) * periods
    pairs = []
    for a in range(periods):
        place = (offset_ref[strip] * (first + a)) & (uv_cols - 1)
        cos, sin = F32(1.0), F32(0.0)
        for digit in range(uv_cols.bit_length() - 1):
            angle = 2.0 * math.pi * (1 << digit) / uv_cols
            by_cos, by_sin = round(math.cos(angle), 15), round(math.sin(angle), 15)
            on = ((place >> digit) & 1) == 1
            cos, sin = (
                jnp.where(on, cos * by_cos - sin * by_sin, cos),
                jnp.where(on, sin * by_cos + cos * by_sin, sin),
            )
        pairs.append((cos, sin))
    return pairs


def spin(place, modulus):
    cos, sin = jnp.ones(place.shape, F32), jnp.zeros(place.shape, F32)
    for digit in range(modulus.bit_length() - 1):
        angle = 2.0 * math.pi * (1 << digit) / modulus
        by_cos, by_sin = round(math.cos(angle), 15), round(math.sin(angle), 15)
        on = ((place >> digit) & 1) == 1
        cos, sin = (
            jnp.where(on, cos * by_cos - sin * by_sin, cos),
            jnp.where(on, sin * by_cos + cos * by_sin, sin),
        )
    return cos, sin


def one_hot(condition):
    return jnp.where(condition, 1.0, 0.0).astype(BF16)


OVER_ROWS = (((0,), (0,)), ((), ()))


def prepare_kernel(
    modulus, rows_each, image_hbm, row_hbm, block_hbm, grid_hbm, offset_hbm, shift_hbm, chosen_hbm,
    folded_ref, phases_ref, spread_ref, weight_ref, other_ref, cos_ref, sin_ref,
    image_ref, row_ref, block_ref, grid_ref, offset_ref, shift_ref, chosen_ref, sems,
):
    core = lax.axis_index("core")
    here = pl.ds(core, 1)
    tile, pieces = 16, 4
    uv_cols = block_ref.shape[1]
    periods = image_ref.shape[0] // STRIP
    quad = (lax.axis_index("y") * GRID["x"] + lax.axis_index("x")) * GRID["zl"] + lax.axis_index("zl")
    first = rows_each * quad
    base = pl.multiple_of((first // tile) * tile, tile)
    pairs = [
        (offset_hbm, offset_ref),
        (shift_hbm, shift_ref),
        (chosen_hbm, chosen_ref),
        (block_hbm, block_ref),
        (grid_hbm.at[:, pl.ds(base, tile), :], grid_ref),
        (row_hbm, row_ref),
    ]
    ahead = len(pairs)
    rows = STRIP // pieces
    for n in range(pieces):
        for a in range(periods):
            at = pl.ds(a * STRIP + n * rows, rows)
            pairs.append((image_hbm.at[at], image_ref.at[at]))
    copies = [pltpu.make_async_copy(*pair, sems.at[n]) for n, pair in enumerate(pairs)]
    for copy in copies:
        copy.start()

    for copy in copies[:4]:
        copy.wait()
    count = shift_ref.shape[1]
    columns = block_ref.shape[2]
    level = lax.broadcasted_iota(I32, (uv_cols, count), 0)
    pick = one_hot(level == shift_ref[here, :])
    row = lax.broadcasted_iota(I32, (count, columns), 1) & (rows_each - 1)
    for part in range(2):
        lines = lax.dot_general(pick, block_ref[part], OVER_ROWS, preferred_element_type=F32)
        for i in range(rows_each):
            at = (part * rows_each + i) * count
            spread_ref[at : at + count, :] = jnp.where(row == i, lines, 0.0).astype(BF16)
    number = lax.broadcasted_iota(I32, (uv_cols, SUB), 0).astype(F32).astype(BF16)
    shift = lax.dot_general(pick, number, OVER_ROWS, preferred_element_type=F32).astype(I32)
    cos_ref[...], sin_ref[...] = spin(
        shift * lax.broadcasted_iota(I32, shift.shape, 1) & (modulus - 1), modulus
    )
    copies[4].wait()
    grids = grid_ref.shape[0]
    grid_rows = jnp.concatenate([grid_ref[g] for g in range(grids)], axis=0)
    line = lax.broadcasted_iota(I32, (grids * tile, count), 0)
    chosen = chosen_ref[here, :] * tile + (first - base)
    for i in range(rows_each):
        pick = one_hot(line == chosen + i)
        weight_ref[i * count : (i + 1) * count, :] = lax.dot_general(
            pick, grid_rows, OVER_ROWS, preferred_element_type=F32
        )

    copies[5].wait()
    step = 16
    b = lax.broadcasted_iota(I32, (1, STRIP), 1)
    cos, sin = spin(offset_ref[core] * b & (modulus - 1), modulus)
    for at in range(0, row_ref.shape[0], step):
        block = slice(at, at + step)
        left = row_ref[block, :STRIP].astype(F32)
        right = row_ref[block, STRIP:].astype(F32)
        phases_ref[block, :STRIP] = (left * cos - right * sin).astype(BF16)
        phases_ref[block, STRIP:] = (right * cos + left * sin).astype(BF16)

    factors = coefficients(core, 1 - core, periods, uv_cols, offset_ref)
    for n, value in enumerate(value for pair in factors for value in pair):
        other_ref[n : n + 1, :] = jnp.full((1, other_ref.shape[1]), value, F32)
    factors = coefficients(core, core, periods, uv_cols, offset_ref)
    width = 512
    for n in range(pieces):
        for a in range(periods):
            copies[ahead + n * periods + a].wait()
        for at in range(n * rows, (n + 1) * rows, step):
            for lane in range(0, image_ref.shape[1], width):
                lanes = slice(lane, lane + width)
                real = imag = 0.0
                for a, (cos, sin) in enumerate(factors):
                    pixels = image_ref[a * STRIP + at : a * STRIP + at + step, lanes].astype(F32)
                    real = real + pixels * cos
                    imag = imag - pixels * sin
                folded_ref[at : at + step, lanes] = real.astype(BF16)
                folded_ref[STRIP + at : STRIP + at + step, lanes] = imag.astype(BF16)


def row_kernel(other_ref, phases_ref, folded_ref, image_ref, out_ref):
    periods = image_ref.shape[0] // STRIP
    step = other_ref.shape[1]
    pairs = [
        (other_ref[2 * a : 2 * a + 1, :], other_ref[2 * a + 1 : 2 * a + 2, :]) for a in range(periods)
    ]
    for lane in range(0, out_ref.shape[1], step):
        lanes = slice(lane, lane + step)
        pixels = [image_ref[a * STRIP : (a + 1) * STRIP, lanes].astype(F32) for a in range(periods)]
        real = folded_ref[:STRIP, lanes].astype(F32)
        imag = folded_ref[STRIP:, lanes].astype(F32)
        for value, (cos, sin) in zip(pixels, pairs):
            real = real + value * cos
            imag = imag - value * sin
        total = jnp.concatenate([real.astype(BF16), imag.astype(BF16)], axis=0)
        out_ref[:, lanes] = jnp.dot(phases_ref[...], total, preferred_element_type=F32).astype(BF16)


def sum_kernel(parts_ref, out_ref):
    ny, nx = GRID["y"], GRID["x"]
    nzl, _, columns = out_ref.shape
    rows = out_ref.shape[1] // nx
    width = 512
    for x in range(nx):
        for zl in range(0, nzl, 2):
            for lane in range(0, columns, width):
                lanes = slice(lane, lane + width)
                here = slice(zl * rows, (zl + 2) * rows)
                total = parts_ref[x, here, lanes].astype(F32)
                for y in range(1, ny):
                    total = total + parts_ref[y * nx + x, here, lanes].astype(F32)
                for n in range(2):
                    out_ref[zl + n, x * rows : (x + 1) * rows, lanes] = total[
                        n * rows : (n + 1) * rows
                    ].astype(BF16)


def middle_kernel(lines, spread_ref, cos_ref, sin_ref, weight_ref, fourier_ref, strip_ref, out_ref):
    nzh, nzl = GRID["zh"], GRID["zl"]
    held = strip_ref.shape[0] // nzh
    blocks = strip_ref.shape[1] // SUB
    pieces = [
        strip_ref[z * held : (z + 1) * held, c * SUB : (c + 1) * SUB]
        for z in range(nzh)
        for c in range(blocks)
    ]
    whole = jnp.concatenate(pieces, axis=0)
    mixed = jnp.dot(spread_ref[...], whole, preferred_element_type=F32)
    repeat = lines // cos_ref.shape[0]
    cos = jnp.concatenate([cos_ref[...]] * repeat, axis=0)
    sin = jnp.concatenate([sin_ref[...]] * repeat, axis=0)
    real, imag = mixed[:lines], mixed[lines:]
    turned = jnp.concatenate([real * cos + imag * sin, imag * cos - real * sin], axis=1)
    spectra = jnp.dot(turned.astype(BF16), fourier_ref[...], preferred_element_type=F32)
    weight = weight_ref[...]
    weighted = jnp.concatenate([spectra[:, :SUB] * weight, -spectra[:, SUB:] * weight], axis=1)
    returned = jnp.dot(weighted.astype(BF16), fourier_ref[...], preferred_element_type=F32)
    real, imag = returned[:, :SUB], -returned[:, SUB:]
    turned = jnp.concatenate([real * cos - imag * sin, imag * cos + real * sin], axis=0)
    inside = held * blocks
    mine = spread_ref[:, pl.ds(pl.multiple_of(lax.axis_index("zh") * inside, inside), inside)]
    back = lax.dot_general(
        mine, turned.astype(BF16), (((0,), (0,)), ((), ())), preferred_element_type=F32
    ).astype(BF16)
    for z in range(nzl):
        for c in range(blocks):
            out_ref[z * held : (z + 1) * held, c * SUB : (c + 1) * SUB] = back[c * held : (c + 1) * held]


def own_kernel(return_ref, cos_ref, sin_ref, image_ref, out_ref, other_ref, own_ref):
    core = lax.axis_index("core")
    step = 16

    def phases(strip, ref):
        turns = jnp.concatenate(
            [cos_ref[pl.ds(strip, 1), :], sin_ref[pl.ds(strip, 1), :]] * 4, axis=0
        )
        turns = jnp.transpose(turns)
        for at in range(0, turns.shape[0], step):
            b = at % STRIP
            cos, sin = turns[at : at + step, 0:1], turns[at : at + step, 1:2]
            ref[at : at + step, :] = (
                return_ref[b : b + step, :].astype(F32) * cos
                + return_ref[STRIP + b : STRIP + b + step, :].astype(F32) * sin
            ).astype(BF16)

    phases(core, own_ref)
    for lane in range(0, out_ref.shape[1], 256):
        lanes = slice(lane, lane + 256)
        out_ref[:, lanes] = jnp.dot(own_ref[...], image_ref[:, lanes], preferred_element_type=F32)
    phases(1 - core, other_ref)


def update_kernel(scale, back_ref, own_ref, image_ref, out_hbm, held_ref, sems):
    step = 256
    copies = []
    for lane in range(0, held_ref.shape[1], step):
        lanes = slice(lane, lane + step)
        other = jnp.dot(back_ref[...], image_ref[:, lanes], preferred_element_type=F32)
        held_ref[:, lanes] = (own_ref[:, lanes] + other) * scale
        at = (slice(None), pl.ds(lane, step))
        copies.append(pltpu.make_async_copy(held_ref.at[at], out_hbm.at[at], sems.at[len(copies)]))
        copies[-1].start()
    for copy in copies:
        copy.wait()


def body(model_image, weight_grids, strip_offsets, subgrid_offsets, grid_index):
    rows_local, facet_width = model_image.shape
    ny, nx, nzl, nzh = (GRID[a] for a in ("y", "x", "zl", "zh"))
    core = lax.axis_index("core")
    modulus = facet_width * nx * nzh
    uv_cols = modulus // SUB
    periods = rows_local // STRIP
    rows_each = STRIP // (nzl * ny * nx)
    count = subgrid_offsets.shape[1]
    strips = strip_offsets.shape[0]
    blocks = facet_width // SUB
    vmem = pl.BlockSpec(memory_space=VMEM)
    half = jax.ShapeDtypeStruct((2 * STRIP, facet_width), BF16)

    hbm = pl.BlockSpec(memory_space=pltpu.HBM)

    swap = [(0, 1), (1, 0)]
    received = lax.ppermute(model_image, "core", swap)

    lines = rows_each * count
    order = np.arange(uv_cols).reshape(nzh, nx, blocks).transpose(0, 2, 1).reshape(-1)
    block = block_tables(order, uv_cols, rows_each)
    square = jax.ShapeDtypeStruct((2 * STRIP, 2 * STRIP), BF16)
    turned = jax.ShapeDtypeStruct((count, SUB), F32)
    grid = jax.ShapeDtypeStruct((weight_grids.shape[0], 16, SUB), BF16)
    sources = (
        model_image, row_table(rows_each), block, weight_grids,
        strip_offsets, subgrid_offsets, grid_index,
    )
    folded, phases, spread, weights, other, cos_d, sin_d = pl.pallas_call(
        functools.partial(prepare_kernel, modulus, rows_each),
        out_shape=(
            half,
            square,
            jax.ShapeDtypeStruct((2 * lines, block.shape[2]), BF16),
            jax.ShapeDtypeStruct((lines, SUB), F32),
            jax.ShapeDtypeStruct((8, 256), F32),
            turned,
            turned,
        ),
        in_specs=[hbm] * len(sources),
        out_specs=(vmem,) * 7,
        scratch_shapes=[VMEM(a.shape, a.dtype) for a in (model_image, square, block, grid)]
        + [
            SMEM(strip_offsets.shape, I32),
            VMEM(subgrid_offsets.shape, I32),
            VMEM(grid_index.shape, I32),
            pltpu.SemaphoreType.DMA((16,)),
        ],
        cost_estimate=pl.CostEstimate(flops=8 * MIB, bytes_accessed=4 * MIB, transcendentals=0),
        compiler_params=grant(12),
        name="prepare",
    )(*(pltpu.with_memory_space_constraint(a, pltpu.HBM) for a in sources))
    partial = pl.pallas_call(
        row_kernel,
        out_shape=half,
        in_specs=[vmem] * 4,
        out_specs=vmem,
        compiler_params=grant(8),
        name="row_transform",
    )(other, phases, folded, received)
    fourier = column_table()
    zl, y = (lax.axis_index(a) for a in ("zl", "y"))
    first = ((zl * ny + y) * GRID["core"] + core) * rows_local
    cos_x, sin_x = turn(
        strip_offsets[:, None] * (first + jnp.arange(rows_local, dtype=I32)[None]), modulus
    )
    partial, fourier = lax.optimization_barrier((partial, fourier))

    parts = lax.all_to_all(
        partial.reshape(ny * nx, -1, facet_width), ("y", "x"), 0, 0, tiled=True
    )
    share = pl.pallas_call(
        sum_kernel,
        out_shape=jax.ShapeDtypeStruct((nzl, nx * 2 * rows_each, facet_width), BF16),
        in_specs=[vmem],
        out_specs=vmem,
        compiler_params=grant(4),
        name="row_sum",
    )(parts)
    parts = lax.all_to_all(share, "zl", 0, 0, tiled=True)
    parts = parts.reshape(nzl, nx * 2 * rows_each, facet_width)
    strip = jnp.sum(parts.astype(F32), axis=0).astype(BF16)
    whole = lax.all_gather(strip, "zh", axis=0, tiled=True)

    back = pl.pallas_call(
        functools.partial(middle_kernel, lines),
        out_shape=jax.ShapeDtypeStruct((nzl * nx * 2 * rows_each, facet_width), BF16),
        in_specs=[vmem] * 6,
        out_specs=vmem,
        compiler_params=grant(16),
        name="subgrids",
    )(spread, cos_d, sin_d, weights, fourier, whole)

    back = back.reshape(nzl, nx * 2 * rows_each, facet_width)
    back = lax.all_to_all(back, "zl", 0, 0, tiled=True)
    back = back.reshape(nzl, nx, 2 * rows_each, facet_width).transpose(1, 0, 2, 3)
    back = jnp.broadcast_to(back[None], (ny, *back.shape))
    back = back.reshape(ny * nx, nzl * 2 * rows_each, facet_width)
    image = lax.all_to_all(back, ("y", "x"), 0, 0, tiled=True).reshape(2 * STRIP, facet_width)

    scale = 1.0 / (modulus * math.sqrt(count * SUB) * math.sqrt(strips * STRIP))
    received = lax.ppermute(image, "core", swap)
    full = jax.ShapeDtypeStruct((rows_local, facet_width), F32)
    own, other_phases = pl.pallas_call(
        own_kernel,
        out_shape=(full, square),
        in_specs=[vmem] * 4,
        out_specs=(vmem, vmem),
        scratch_shapes=[VMEM(square.shape, BF16)],
        cost_estimate=pl.CostEstimate(flops=512 * MIB, bytes_accessed=MIB, transcendentals=0),
        compiler_params=grant(8),
        name="own_part",
    )(return_table(rows_each), cos_x, sin_x, image)
    return pl.pallas_call(
        functools.partial(update_kernel, scale),
        out_shape=full,
        in_specs=[vmem] * 3,
        out_specs=hbm,
        scratch_shapes=[VMEM(full.shape, F32), pltpu.SemaphoreType.DMA((8,))],
        compiler_params=grant(8),
        name="update",
    )(other_phases, own, received)


def solution(mesh):
    finer = Mesh(mesh.devices.reshape(tuple(GRID.values())), tuple(GRID))
    rows, cols = ("zl", "y", "core"), ("zh", "x")
    return jax.shard_map(
        body,
        mesh=finer,
        in_specs=(P(rows, cols), P(), P(), P(), P()),
        out_specs=P(rows, cols),
        check_vma=False,
    )
```

```python
import functools
import math

import jax
import jax.numpy as jnp
import ml_dtypes
import numpy as np
from jax import lax
from jax.experimental import pallas as pl
from jax.experimental.pallas import tpu as pltpu
from jax.sharding import Mesh
from jax.sharding import PartitionSpec as P

F32 = jnp.float32
BF16 = jnp.bfloat16
I32 = jnp.int32
STRIP = 256
SUB = 256
GRID = {"zl": 4, "y": 4, "core": 2, "zh": 4, "x": 4}
FIRST = ("zl", "y", "core")
SECOND = ("zl", "y", "core", "x")
VMEM = pltpu.VMEM
SMEM = pltpu.SMEM
MIB = 1 << 20


def grant(mib):
    return pltpu.CompilerParams(vmem_limit_bytes=mib * MIB)


def groups(axes):
    place = np.arange(math.prod(GRID[a] for a in axes)).reshape([GRID[a] for a in axes])
    lists = []
    for core in range(GRID["core"]):
        along_y = (core == 0) == (axes == FIRST)
        part = place[:, :, core] if along_y else place[:, :, core].swapaxes(0, 1)
        lists += [row.reshape(-1).tolist() for row in part]
    return lists


def exchange(value, axes):
    return lax.all_to_all(value, axes, 0, 0, axis_index_groups=groups(axes), tiled=True)


def turn(numerator, denominator):
    angle = (numerator % denominator).astype(F32) * (2.0 * math.pi / denominator)
    return jnp.cos(angle), jnp.sin(angle)


def fixed(values):
    return jnp.asarray(np.asarray(values, dtype=ml_dtypes.bfloat16))


def row_table(rows_each):
    r = np.arange(STRIP).reshape(-1, 1, rows_each, 1, 1)
    p = np.arange(2).reshape(1, 2, 1, 1, 1)
    q = np.arange(2).reshape(1, 1, 1, 2, 1)
    b = np.arange(STRIP).reshape(1, 1, 1, 1, -1)
    phase = 2.0 * np.pi * ((r * b) % STRIP) / STRIP + (p - q) * (np.pi / 2)
    return fixed(np.cos(phase.reshape(2 * STRIP, 2 * STRIP)))


def return_table(rows_each):
    b = np.arange(STRIP).reshape(-1, 1, 1, 1)
    r = np.arange(STRIP).reshape(1, -1, 1, rows_each)
    p = np.arange(2).reshape(1, 1, 2, 1)
    phase = (2.0 * np.pi * ((r * b) % STRIP) / STRIP + p * (np.pi / 2)).reshape(STRIP, 2 * STRIP)
    return fixed(np.concatenate([np.cos(phase), -np.sin(phase)], axis=0))


def column_table():
    d = np.arange(SUB)
    phase = 2.0 * np.pi * (np.outer(d, d) % SUB) / SUB
    cos, sin = np.cos(phase), np.sin(phase)
    return fixed(np.block([[cos, -sin], [sin, cos]]))


def block_tables(order, uv_cols, rows_each):
    u = np.arange(uv_cols).reshape(1, -1, 1, 1, 1, 1)
    p = np.arange(2).reshape(2, 1, 1, 1, 1, 1)
    c = order.reshape(1, 1, -1, 1, 1, 1)
    q = np.arange(2).reshape(1, 1, 1, 2, 1, 1)
    phase = 2.0 * np.pi * ((u * c) % uv_cols) / uv_cols + (p - q) * (np.pi / 2)
    table = np.broadcast_to(np.cos(phase), (2, uv_cols, order.size, 2, rows_each, 1))
    return fixed(table.reshape(2, uv_cols, -1))


def coefficients(strip, rows_of, periods, uv_cols, offset_ref):
    zl, y = (lax.axis_index(a) for a in ("zl", "y"))
    first = ((zl * GRID["y"] + y) * GRID["core"] + rows_of) * periods
    pairs = []
    for a in range(periods):
        place = (offset_ref[strip] * (first + a)) & (uv_cols - 1)
        cos, sin = F32(1.0), F32(0.0)
        for digit in range(uv_cols.bit_length() - 1):
            angle = 2.0 * math.pi * (1 << digit) / uv_cols
            by_cos, by_sin = round(math.cos(angle), 15), round(math.sin(angle), 15)
            on = ((place >> digit) & 1) == 1
            cos, sin = (
                jnp.where(on, cos * by_cos - sin * by_sin, cos),
                jnp.where(on, sin * by_cos + cos * by_sin, sin),
            )
        pairs.append((cos, sin))
    return pairs


def spin(place, modulus):
    cos, sin = jnp.ones(place.shape, F32), jnp.zeros(place.shape, F32)
    for digit in range(modulus.bit_length() - 1):
        angle = 2.0 * math.pi * (1 << digit) / modulus
        by_cos, by_sin = round(math.cos(angle), 15), round(math.sin(angle), 15)
        on = ((place >> digit) & 1) == 1
        cos, sin = (
            jnp.where(on, cos * by_cos - sin * by_sin, cos),
            jnp.where(on, sin * by_cos + cos * by_sin, sin),
        )
    return cos, sin


def one_hot(condition):
    return jnp.where(condition, 1.0, 0.0).astype(BF16)


OVER_ROWS = (((0,), (0,)), ((), ()))


def prepare_kernel(
    modulus, rows_each, image_hbm, row_hbm, block_hbm, grid_hbm, offset_hbm, shift_hbm, chosen_hbm,
    folded_ref, phases_ref, spread_ref, weight_ref, other_ref, cos_ref, sin_ref,
    image_ref, row_ref, block_ref, grid_ref, offset_ref, shift_ref, chosen_ref, sems,
):
    core = lax.axis_index("core")
    here = pl.ds(core, 1)
    tile, pieces = 16, 4
    uv_cols = block_ref.shape[1]
    periods = image_ref.shape[0] // STRIP
    y, zl = lax.axis_index("y"), lax.axis_index("zl")
    early, late = jnp.where(core == 0, y, zl), jnp.where(core == 0, zl, y)
    quad = (early * GRID["zl"] + late) * GRID["x"] + lax.axis_index("x")
    first = rows_each * quad
    base = pl.multiple_of((first // tile) * tile, tile)
    pairs = [
        (offset_hbm, offset_ref),
        (shift_hbm, shift_ref),
        (chosen_hbm, chosen_ref),
        (block_hbm, block_ref),
        (grid_hbm.at[:, pl.ds(base, tile), :], grid_ref),
        (row_hbm, row_ref),
    ]
    ahead = len(pairs)
    rows = STRIP // pieces
    for n in range(pieces):
        for a in range(periods):
            at = pl.ds(a * STRIP + n * rows, rows)
            pairs.append((image_hbm.at[at], image_ref.at[at]))
    copies = [pltpu.make_async_copy(*pair, sems.at[n]) for n, pair in enumerate(pairs)]
    for copy in copies:
        copy.start()

    for copy in copies[:4]:
        copy.wait()
    count = shift_ref.shape[1]
    columns = block_ref.shape[2]
    level = lax.broadcasted_iota(I32, (uv_cols, count), 0)
    pick = one_hot(level == shift_ref[here, :])
    row = lax.broadcasted_iota(I32, (count, columns), 1) & (rows_each - 1)
    for part in range(2):
        lines = lax.dot_general(pick, block_ref[part], OVER_ROWS, preferred_element_type=F32)
        for i in range(rows_each):
            at = (part * rows_each + i) * count
            spread_ref[at : at + count, :] = jnp.where(row == i, lines, 0.0).astype(BF16)
    number = lax.broadcasted_iota(I32, (uv_cols, SUB), 0).astype(F32).astype(BF16)
    shift = lax.dot_general(pick, number, OVER_ROWS, preferred_element_type=F32).astype(I32)
    cos_ref[...], sin_ref[...] = spin(
        shift * lax.broadcasted_iota(I32, shift.shape, 1) & (modulus - 1), modulus
    )
    copies[4].wait()
    grids = grid_ref.shape[0]
    grid_rows = jnp.concatenate([grid_ref[g] for g in range(grids)], axis=0)
    line = lax.broadcasted_iota(I32, (grids * tile, count), 0)
    chosen = chosen_ref[here, :] * tile + (first - base)
    for i in range(rows_each):
        pick = one_hot(line == chosen + i)
        weight_ref[i * count : (i + 1) * count, :] = lax.dot_general(
            pick, grid_rows, OVER_ROWS, preferred_element_type=F32
        )

    copies[5].wait()
    step = 16
    b = lax.broadcasted_iota(I32, (1, STRIP), 1)
    cos, sin = spin(offset_ref[core] * b & (modulus - 1), modulus)
    for at in range(0, row_ref.shape[0], step):
        block = slice(at, at + step)
        left = row_ref[block, :STRIP].astype(F32)
        right = row_ref[block, STRIP:].astype(F32)
        phases_ref[block, :STRIP] = (left * cos - right * sin).astype(BF16)
        phases_ref[block, STRIP:] = (right * cos + left * sin).astype(BF16)

    factors = coefficients(core, 1 - core, periods, uv_cols, offset_ref)
    for n, value in enumerate(value for pair in factors for value in pair):
        other_ref[n : n + 1, :] = jnp.full((1, other_ref.shape[1]), value, F32)
    factors = coefficients(core, core, periods, uv_cols, offset_ref)
    width = 512
    for n in range(pieces):
        for a in range(periods):
            copies[ahead + n * periods + a].wait()
        for at in range(n * rows, (n + 1) * rows, step):
            for lane in range(0, image_ref.shape[1], width):
                lanes = slice(lane, lane + width)
                real = imag = 0.0
                for a, (cos, sin) in enumerate(factors):
                    pixels = image_ref[a * STRIP + at : a * STRIP + at + step, lanes].astype(F32)
                    real = real + pixels * cos
                    imag = imag - pixels * sin
                folded_ref[at : at + step, lanes] = real.astype(BF16)
                folded_ref[STRIP + at : STRIP + at + step, lanes] = imag.astype(BF16)


def row_kernel(other_ref, phases_ref, folded_ref, image_ref, out_ref):
    periods = image_ref.shape[0] // STRIP
    step = other_ref.shape[1]
    pairs = [
        (other_ref[2 * a : 2 * a + 1, :], other_ref[2 * a + 1 : 2 * a + 2, :]) for a in range(periods)
    ]
    for lane in range(0, out_ref.shape[1], step):
        lanes = slice(lane, lane + step)
        pixels = [image_ref[a * STRIP : (a + 1) * STRIP, lanes].astype(F32) for a in range(periods)]
        real = folded_ref[:STRIP, lanes].astype(F32)
        imag = folded_ref[STRIP:, lanes].astype(F32)
        for value, (cos, sin) in zip(pixels, pairs):
            real = real + value * cos
            imag = imag - value * sin
        total = jnp.concatenate([real.astype(BF16), imag.astype(BF16)], axis=0)
        out_ref[:, lanes] = jnp.dot(phases_ref[...], total, preferred_element_type=F32).astype(BF16)


def sum_kernel(parts_ref, out_ref):
    step, width = 16, 512
    for at in range(0, out_ref.shape[0], step):
        for lane in range(0, out_ref.shape[1], width):
            here = (slice(at, at + step), slice(lane, lane + width))
            total = parts_ref[(0, *here)].astype(F32)
            for n in range(1, parts_ref.shape[0]):
                total = total + parts_ref[(n, *here)].astype(F32)
            out_ref[here] = total.astype(BF16)


def middle_kernel(lines, spread_ref, cos_ref, sin_ref, weight_ref, fourier_ref, strip_ref, out_ref):
    nzh, nzl = GRID["zh"], GRID["zl"]
    held = strip_ref.shape[0] // nzh
    blocks = strip_ref.shape[1] // SUB
    pieces = [
        strip_ref[z * held : (z + 1) * held, c * SUB : (c + 1) * SUB]
        for z in range(nzh)
        for c in range(blocks)
    ]
    whole = jnp.concatenate(pieces, axis=0)
    mixed = jnp.dot(spread_ref[...], whole, preferred_element_type=F32)
    repeat = lines // cos_ref.shape[0]
    cos = jnp.concatenate([cos_ref[...]] * repeat, axis=0)
    sin = jnp.concatenate([sin_ref[...]] * repeat, axis=0)
    real, imag = mixed[:lines], mixed[lines:]
    turned = jnp.concatenate([real * cos + imag * sin, imag * cos - real * sin], axis=1)
    spectra = jnp.dot(turned.astype(BF16), fourier_ref[...], preferred_element_type=F32)
    weight = weight_ref[...]
    weighted = jnp.concatenate([spectra[:, :SUB] * weight, -spectra[:, SUB:] * weight], axis=1)
    returned = jnp.dot(weighted.astype(BF16), fourier_ref[...], preferred_element_type=F32)
    real, imag = returned[:, :SUB], -returned[:, SUB:]
    turned = jnp.concatenate([real * cos - imag * sin, imag * cos + real * sin], axis=0)
    inside = held * blocks
    mine = spread_ref[:, pl.ds(pl.multiple_of(lax.axis_index("zh") * inside, inside), inside)]
    back = lax.dot_general(
        mine, turned.astype(BF16), (((0,), (0,)), ((), ())), preferred_element_type=F32
    ).astype(BF16)
    for z in range(nzl):
        for c in range(blocks):
            out_ref[z * held : (z + 1) * held, c * SUB : (c + 1) * SUB] = back[c * held : (c + 1) * held]


def own_kernel(return_ref, cos_ref, sin_ref, image_ref, out_ref, other_ref, own_ref):
    core = lax.axis_index("core")
    step = 16

    def phases(strip, ref):
        turns = jnp.concatenate(
            [cos_ref[pl.ds(strip, 1), :], sin_ref[pl.ds(strip, 1), :]] * 4, axis=0
        )
        turns = jnp.transpose(turns)
        for at in range(0, turns.shape[0], step):
            b = at % STRIP
            cos, sin = turns[at : at + step, 0:1], turns[at : at + step, 1:2]
            ref[at : at + step, :] = (
                return_ref[b : b + step, :].astype(F32) * cos
                + return_ref[STRIP + b : STRIP + b + step, :].astype(F32) * sin
            ).astype(BF16)

    phases(core, own_ref)
    for lane in range(0, out_ref.shape[1], 256):
        lanes = slice(lane, lane + 256)
        out_ref[:, lanes] = jnp.dot(own_ref[...], image_ref[:, lanes], preferred_element_type=F32)
    phases(1 - core, other_ref)


def update_kernel(scale, back_ref, own_ref, image_ref, out_hbm, held_ref, sems):
    step = 256
    copies = []
    for lane in range(0, held_ref.shape[1], step):
        lanes = slice(lane, lane + step)
        other = jnp.dot(back_ref[...], image_ref[:, lanes], preferred_element_type=F32)
        held_ref[:, lanes] = (own_ref[:, lanes] + other) * scale
        at = (slice(None), pl.ds(lane, step))
        copies.append(pltpu.make_async_copy(held_ref.at[at], out_hbm.at[at], sems.at[len(copies)]))
        copies[-1].start()
    for copy in copies:
        copy.wait()


def body(model_image, weight_grids, strip_offsets, subgrid_offsets, grid_index):
    rows_local, facet_width = model_image.shape
    ny, nx, nzl, nzh = (GRID[a] for a in ("y", "x", "zl", "zh"))
    core = lax.axis_index("core")
    modulus = facet_width * nx * nzh
    uv_cols = modulus // SUB
    periods = rows_local // STRIP
    rows_each = STRIP // (nzl * ny * nx)
    count = subgrid_offsets.shape[1]
    strips = strip_offsets.shape[0]
    blocks = facet_width // SUB
    vmem = pl.BlockSpec(memory_space=VMEM)
    half = jax.ShapeDtypeStruct((2 * STRIP, facet_width), BF16)

    hbm = pl.BlockSpec(memory_space=pltpu.HBM)

    swap = [(0, 1), (1, 0)]
    received = lax.ppermute(model_image, "core", swap)

    lines = rows_each * count
    order = np.arange(uv_cols).reshape(nzh, nx, blocks).transpose(0, 2, 1).reshape(-1)
    block = block_tables(order, uv_cols, rows_each)
    square = jax.ShapeDtypeStruct((2 * STRIP, 2 * STRIP), BF16)
    turned = jax.ShapeDtypeStruct((count, SUB), F32)
    grid = jax.ShapeDtypeStruct((weight_grids.shape[0], 16, SUB), BF16)
    sources = (
        model_image, row_table(rows_each), block, weight_grids,
        strip_offsets, subgrid_offsets, grid_index,
    )
    folded, phases, spread, weights, other, cos_d, sin_d = pl.pallas_call(
        functools.partial(prepare_kernel, modulus, rows_each),
        out_shape=(
            half,
            square,
            jax.ShapeDtypeStruct((2 * lines, block.shape[2]), BF16),
            jax.ShapeDtypeStruct((lines, SUB), F32),
            jax.ShapeDtypeStruct((8, 256), F32),
            turned,
            turned,
        ),
        in_specs=[hbm] * len(sources),
        out_specs=(vmem,) * 7,
        scratch_shapes=[VMEM(a.shape, a.dtype) for a in (model_image, square, block, grid)]
        + [
            SMEM(strip_offsets.shape, I32),
            VMEM(subgrid_offsets.shape, I32),
            VMEM(grid_index.shape, I32),
            pltpu.SemaphoreType.DMA((16,)),
        ],
        cost_estimate=pl.CostEstimate(flops=8 * MIB, bytes_accessed=4 * MIB, transcendentals=0),
        compiler_params=grant(12),
        name="prepare",
    )(*(pltpu.with_memory_space_constraint(a, pltpu.HBM) for a in sources))
    partial = pl.pallas_call(
        row_kernel,
        out_shape=half,
        in_specs=[vmem] * 4,
        out_specs=vmem,
        compiler_params=grant(8),
        name="row_transform",
    )(other, phases, folded, received)
    fourier = column_table()
    zl, y = (lax.axis_index(a) for a in ("zl", "y"))
    first = ((zl * ny + y) * GRID["core"] + core) * rows_local
    cos_x, sin_x = turn(
        strip_offsets[:, None] * (first + jnp.arange(rows_local, dtype=I32)[None]), modulus
    )
    partial, fourier = lax.optimization_barrier((partial, fourier))

    parts = exchange(partial.reshape(ny, -1, facet_width), FIRST)
    share = pl.pallas_call(
        sum_kernel,
        out_shape=jax.ShapeDtypeStruct(parts.shape[1:], BF16),
        in_specs=[vmem],
        out_specs=vmem,
        compiler_params=grant(4),
        name="row_sum",
    )(parts)
    parts = exchange(share.reshape(nzl * nx, 2 * rows_each, facet_width), SECOND)
    parts = parts.reshape(nzl, nx * 2 * rows_each, facet_width)
    strip = jnp.sum(parts.astype(F32), axis=0).astype(BF16)
    whole = lax.all_gather(strip, "zh", axis=0, tiled=True)

    back = pl.pallas_call(
        functools.partial(middle_kernel, lines),
        out_shape=jax.ShapeDtypeStruct((nzl * nx * 2 * rows_each, facet_width), BF16),
        in_specs=[vmem] * 6,
        out_specs=vmem,
        compiler_params=grant(16),
        name="subgrids",
    )(spread, cos_d, sin_d, weights, fourier, whole)

    back = back.reshape(nzl * nx, 2 * rows_each, facet_width)
    back = exchange(back, SECOND).reshape(1, -1, facet_width)
    back = jnp.broadcast_to(back, (ny, *back.shape[1:]))
    image = exchange(back, FIRST).reshape(2 * STRIP, facet_width)

    scale = 1.0 / (modulus * math.sqrt(count * SUB) * math.sqrt(strips * STRIP))
    received = lax.ppermute(image, "core", swap)
    full = jax.ShapeDtypeStruct((rows_local, facet_width), F32)
    own, other_phases = pl.pallas_call(
        own_kernel,
        out_shape=(full, square),
        in_specs=[vmem] * 4,
        out_specs=(vmem, vmem),
        scratch_shapes=[VMEM(square.shape, BF16)],
        cost_estimate=pl.CostEstimate(flops=512 * MIB, bytes_accessed=MIB, transcendentals=0),
        compiler_params=grant(8),
        name="own_part",
    )(return_table(rows_each), cos_x, sin_x, image)
    return pl.pallas_call(
        functools.partial(update_kernel, scale),
        out_shape=full,
        in_specs=[vmem] * 3,
        out_specs=hbm,
        scratch_shapes=[VMEM(full.shape, F32), pltpu.SemaphoreType.DMA((8,))],
        compiler_params=grant(8),
        name="update",
    )(other_phases, own, received)


def solution(mesh):
    finer = Mesh(mesh.devices.reshape(tuple(GRID.values())), tuple(GRID))
    rows, cols = ("zl", "y", "core"), ("zh", "x")
    return jax.shard_map(
        body,
        mesh=finer,
        in_specs=(P(rows, cols), P(), P(), P(), P()),
        out_specs=P(rows, cols),
        check_vma=False,
    )
```

```python
import functools
import math

import jax
import jax.numpy as jnp
import ml_dtypes
import numpy as np
from jax import lax
from jax.experimental import pallas as pl
from jax.experimental.pallas import tpu as pltpu
from jax.sharding import Mesh
from jax.sharding import PartitionSpec as P

F32 = jnp.float32
BF16 = jnp.bfloat16
I32 = jnp.int32
STRIP = 256
SUB = 256
GRID = {"zl": 4, "y": 4, "core": 2, "zh": 4, "x": 4}
FIRST = ("zl", "y", "core")
SECOND = ("zl", "y", "core", "x")
VMEM = pltpu.VMEM
SMEM = pltpu.SMEM
MIB = 1 << 20


def grant(mib):
    return pltpu.CompilerParams(vmem_limit_bytes=mib * MIB)


def groups(axes):
    place = np.arange(math.prod(GRID[a] for a in axes)).reshape([GRID[a] for a in axes])
    lists = []
    for core in range(GRID["core"]):
        along_y = (core == 0) == (axes == FIRST)
        part = place[:, :, core] if along_y else place[:, :, core].swapaxes(0, 1)
        lists += [row.T.reshape(-1).tolist() for row in part]
    return lists


def exchange(value, axes):
    return lax.all_to_all(value, axes, 0, 0, axis_index_groups=groups(axes), tiled=True)


def turn(numerator, denominator):
    angle = (numerator % denominator).astype(F32) * (2.0 * math.pi / denominator)
    return jnp.cos(angle), jnp.sin(angle)


def fixed(values):
    return jnp.asarray(np.asarray(values, dtype=ml_dtypes.bfloat16))


def row_table(rows_each):
    r = np.arange(STRIP).reshape(-1, 1, rows_each, 1, 1)
    p = np.arange(2).reshape(1, 2, 1, 1, 1)
    q = np.arange(2).reshape(1, 1, 1, 2, 1)
    b = np.arange(STRIP).reshape(1, 1, 1, 1, -1)
    phase = 2.0 * np.pi * ((r * b) % STRIP) / STRIP + (p - q) * (np.pi / 2)
    return fixed(np.cos(phase.reshape(2 * STRIP, 2 * STRIP)))


def return_table(rows_each):
    b = np.arange(STRIP).reshape(-1, 1, 1, 1)
    r = np.arange(STRIP).reshape(1, -1, 1, rows_each)
    p = np.arange(2).reshape(1, 1, 2, 1)
    phase = (2.0 * np.pi * ((r * b) % STRIP) / STRIP + p * (np.pi / 2)).reshape(STRIP, 2 * STRIP)
    return fixed(np.concatenate([np.cos(phase), -np.sin(phase)], axis=0))


def column_table():
    d = np.arange(SUB)
    phase = 2.0 * np.pi * (np.outer(d, d) % SUB) / SUB
    cos, sin = np.cos(phase), np.sin(phase)
    return fixed(np.block([[cos, -sin], [sin, cos]]))


def block_tables(order, uv_cols, rows_each):
    u = np.arange(uv_cols).reshape(1, -1, 1, 1, 1, 1)
    p = np.arange(2).reshape(2, 1, 1, 1, 1, 1)
    c = order.reshape(1, 1, -1, 1, 1, 1)
    q = np.arange(2).reshape(1, 1, 1, 2, 1, 1)
    phase = 2.0 * np.pi * ((u * c) % uv_cols) / uv_cols + (p - q) * (np.pi / 2)
    table = np.broadcast_to(np.cos(phase), (2, uv_cols, order.size, 2, rows_each, 1))
    return fixed(table.reshape(2, uv_cols, -1))


def coefficients(strip, rows_of, periods, uv_cols, offset_ref):
    zl, y = (lax.axis_index(a) for a in ("zl", "y"))
    first = ((zl * GRID["y"] + y) * GRID["core"] + rows_of) * periods
    pairs = []
    for a in range(periods):
        place = (offset_ref[strip] * (first + a)) & (uv_cols - 1)
        cos, sin = F32(1.0), F32(0.0)
        for digit in range(uv_cols.bit_length() - 1):
            angle = 2.0 * math.pi * (1 << digit) / uv_cols
            by_cos, by_sin = round(math.cos(angle), 15), round(math.sin(angle), 15)
            on = ((place >> digit) & 1) == 1
            cos, sin = (
                jnp.where(on, cos * by_cos - sin * by_sin, cos),
                jnp.where(on, sin * by_cos + cos * by_sin, sin),
            )
        pairs.append((cos, sin))
    return pairs


def spin(place, modulus):
    cos, sin = jnp.ones(place.shape, F32), jnp.zeros(place.shape, F32)
    for digit in range(modulus.bit_length() - 1):
        angle = 2.0 * math.pi * (1 << digit) / modulus
        by_cos, by_sin = round(math.cos(angle), 15), round(math.sin(angle), 15)
        on = ((place >> digit) & 1) == 1
        cos, sin = (
            jnp.where(on, cos * by_cos - sin * by_sin, cos),
            jnp.where(on, sin * by_cos + cos * by_sin, sin),
        )
    return cos, sin


def one_hot(condition):
    return jnp.where(condition, 1.0, 0.0).astype(BF16)


OVER_ROWS = (((0,), (0,)), ((), ()))


def prepare_kernel(
    modulus, rows_each, image_hbm, row_hbm, block_hbm, grid_hbm, offset_hbm, shift_hbm, chosen_hbm,
    folded_ref, phases_ref, spread_ref, weight_ref, other_ref, cos_ref, sin_ref,
    image_ref, row_ref, block_ref, grid_ref, offset_ref, shift_ref, chosen_ref, sems,
):
    core = lax.axis_index("core")
    here = pl.ds(core, 1)
    tile, pieces = 16, 4
    uv_cols = block_ref.shape[1]
    periods = image_ref.shape[0] // STRIP
    y, zl = lax.axis_index("y"), lax.axis_index("zl")
    early, late = jnp.where(core == 0, y, zl), jnp.where(core == 0, zl, y)
    quad = (early * GRID["x"] + lax.axis_index("x")) * GRID["zl"] + late
    first = rows_each * quad
    base = pl.multiple_of((first // tile) * tile, tile)
    pairs = [
        (offset_hbm, offset_ref),
        (shift_hbm, shift_ref),
        (chosen_hbm, chosen_ref),
        (block_hbm, block_ref),
        (grid_hbm.at[:, pl.ds(base, tile), :], grid_ref),
        (row_hbm, row_ref),
    ]
    ahead = len(pairs)
    rows = STRIP // pieces
    for n in range(pieces):
        for a in range(periods):
            at = pl.ds(a * STRIP + n * rows, rows)
            pairs.append((image_hbm.at[at], image_ref.at[at]))
    copies = [pltpu.make_async_copy(*pair, sems.at[n]) for n, pair in enumerate(pairs)]
    for copy in copies:
        copy.start()

    for copy in copies[:4]:
        copy.wait()
    count = shift_ref.shape[1]
    columns = block_ref.shape[2]
    level = lax.broadcasted_iota(I32, (uv_cols, count), 0)
    pick = one_hot(level == shift_ref[here, :])
    row = lax.broadcasted_iota(I32, (count, columns), 1) & (rows_each - 1)
    for part in range(2):
        lines = lax.dot_general(pick, block_ref[part], OVER_ROWS, preferred_element_type=F32)
        for i in range(rows_each):
            at = (part * rows_each + i) * count
            spread_ref[at : at + count, :] = jnp.where(row == i, lines, 0.0).astype(BF16)
    number = lax.broadcasted_iota(I32, (uv_cols, SUB), 0).astype(F32).astype(BF16)
    shift = lax.dot_general(pick, number, OVER_ROWS, preferred_element_type=F32).astype(I32)
    cos_ref[...], sin_ref[...] = spin(
        shift * lax.broadcasted_iota(I32, shift.shape, 1) & (modulus - 1), modulus
    )
    copies[4].wait()
    grids = grid_ref.shape[0]
    grid_rows = jnp.concatenate([grid_ref[g] for g in range(grids)], axis=0)
    line = lax.broadcasted_iota(I32, (grids * tile, count), 0)
    chosen = chosen_ref[here, :] * tile + (first - base)
    for i in range(rows_each):
        pick = one_hot(line == chosen + i)
        weight_ref[i * count : (i + 1) * count, :] = lax.dot_general(
            pick, grid_rows, OVER_ROWS, preferred_element_type=F32
        )

    copies[5].wait()
    step = 16
    b = lax.broadcasted_iota(I32, (1, STRIP), 1)
    cos, sin = spin(offset_ref[core] * b & (modulus - 1), modulus)
    for at in range(0, row_ref.shape[0], step):
        block = slice(at, at + step)
        left = row_ref[block, :STRIP].astype(F32)
        right = row_ref[block, STRIP:].astype(F32)
        phases_ref[block, :STRIP] = (left * cos - right * sin).astype(BF16)
        phases_ref[block, STRIP:] = (right * cos + left * sin).astype(BF16)

    factors = coefficients(core, 1 - core, periods, uv_cols, offset_ref)
    for n, value in enumerate(value for pair in factors for value in pair):
        other_ref[n : n + 1, :] = jnp.full((1, other_ref.shape[1]), value, F32)
    factors = coefficients(core, core, periods, uv_cols, offset_ref)
    width = 512
    for n in range(pieces):
        for a in range(periods):
            copies[ahead + n * periods + a].wait()
        for at in range(n * rows, (n + 1) * rows, step):
            for lane in range(0, image_ref.shape[1], width):
                lanes = slice(lane, lane + width)
                real = imag = 0.0
                for a, (cos, sin) in enumerate(factors):
                    pixels = image_ref[a * STRIP + at : a * STRIP + at + step, lanes].astype(F32)
                    real = real + pixels * cos
                    imag = imag - pixels * sin
                folded_ref[at : at + step, lanes] = real.astype(BF16)
                folded_ref[STRIP + at : STRIP + at + step, lanes] = imag.astype(BF16)


def row_kernel(other_ref, phases_ref, folded_ref, image_ref, out_ref):
    periods = image_ref.shape[0] // STRIP
    step = other_ref.shape[1]
    pairs = [
        (other_ref[2 * a : 2 * a + 1, :], other_ref[2 * a + 1 : 2 * a + 2, :]) for a in range(periods)
    ]
    for lane in range(0, out_ref.shape[1], step):
        lanes = slice(lane, lane + step)
        pixels = [image_ref[a * STRIP : (a + 1) * STRIP, lanes].astype(F32) for a in range(periods)]
        real = folded_ref[:STRIP, lanes].astype(F32)
        imag = folded_ref[STRIP:, lanes].astype(F32)
        for value, (cos, sin) in zip(pixels, pairs):
            real = real + value * cos
            imag = imag - value * sin
        total = jnp.concatenate([real.astype(BF16), imag.astype(BF16)], axis=0)
        out_ref[:, lanes] = jnp.dot(phases_ref[...], total, preferred_element_type=F32).astype(BF16)


def sum_kernel(parts_ref, out_ref):
    step, width = 16, 512
    for at in range(0, out_ref.shape[0], step):
        for lane in range(0, out_ref.shape[1], width):
            here = (slice(at, at + step), slice(lane, lane + width))
            total = parts_ref[(0, *here)].astype(F32)
            for n in range(1, parts_ref.shape[0]):
                total = total + parts_ref[(n, *here)].astype(F32)
            out_ref[here] = total.astype(BF16)


def middle_kernel(lines, spread_ref, cos_ref, sin_ref, weight_ref, fourier_ref, strip_ref, out_ref):
    nzh = GRID["zh"]
    held = strip_ref.shape[0] // nzh
    blocks = strip_ref.shape[1] // SUB
    pieces = [
        strip_ref[z * held : (z + 1) * held, c * SUB : (c + 1) * SUB]
        for z in range(nzh)
        for c in range(blocks)
    ]
    whole = jnp.concatenate(pieces, axis=0)
    mixed = jnp.dot(spread_ref[...], whole, preferred_element_type=F32)
    repeat = lines // cos_ref.shape[0]
    cos = jnp.concatenate([cos_ref[...]] * repeat, axis=0)
    sin = jnp.concatenate([sin_ref[...]] * repeat, axis=0)
    real, imag = mixed[:lines], mixed[lines:]
    turned = jnp.concatenate([real * cos + imag * sin, imag * cos - real * sin], axis=1)
    spectra = jnp.dot(turned.astype(BF16), fourier_ref[...], preferred_element_type=F32)
    weight = weight_ref[...]
    weighted = jnp.concatenate([spectra[:, :SUB] * weight, -spectra[:, SUB:] * weight], axis=1)
    returned = jnp.dot(weighted.astype(BF16), fourier_ref[...], preferred_element_type=F32)
    real, imag = returned[:, :SUB], -returned[:, SUB:]
    turned = jnp.concatenate([real * cos - imag * sin, imag * cos + real * sin], axis=0)
    inside = held * blocks
    mine = spread_ref[:, pl.ds(pl.multiple_of(lax.axis_index("zh") * inside, inside), inside)]
    back = lax.dot_general(
        mine, turned.astype(BF16), (((0,), (0,)), ((), ())), preferred_element_type=F32
    ).astype(BF16)
    for c in range(blocks):
        out_ref[:, c * SUB : (c + 1) * SUB] = back[c * held : (c + 1) * held]


def own_kernel(return_ref, cos_ref, sin_ref, image_ref, out_ref, other_ref, own_ref):
    core = lax.axis_index("core")
    step = 16

    def phases(strip, ref):
        turns = jnp.concatenate(
            [cos_ref[pl.ds(strip, 1), :], sin_ref[pl.ds(strip, 1), :]] * 4, axis=0
        )
        turns = jnp.transpose(turns)
        for at in range(0, turns.shape[0], step):
            b = at % STRIP
            cos, sin = turns[at : at + step, 0:1], turns[at : at + step, 1:2]
            ref[at : at + step, :] = (
                return_ref[b : b + step, :].astype(F32) * cos
                + return_ref[STRIP + b : STRIP + b + step, :].astype(F32) * sin
            ).astype(BF16)

    phases(core, own_ref)
    for lane in range(0, out_ref.shape[1], 256):
        lanes = slice(lane, lane + 256)
        out_ref[:, lanes] = jnp.dot(own_ref[...], image_ref[:, lanes], preferred_element_type=F32)
    phases(1 - core, other_ref)


def update_kernel(scale, back_ref, own_ref, image_ref, out_hbm, held_ref, sems):
    step = 256
    copies = []
    for lane in range(0, held_ref.shape[1], step):
        lanes = slice(lane, lane + step)
        other = jnp.dot(back_ref[...], image_ref[:, lanes], preferred_element_type=F32)
        held_ref[:, lanes] = (own_ref[:, lanes] + other) * scale
        at = (slice(None), pl.ds(lane, step))
        copies.append(pltpu.make_async_copy(held_ref.at[at], out_hbm.at[at], sems.at[len(copies)]))
        copies[-1].start()
    for copy in copies:
        copy.wait()


def body(model_image, weight_grids, strip_offsets, subgrid_offsets, grid_index):
    rows_local, facet_width = model_image.shape
    ny, nx, nzl, nzh = (GRID[a] for a in ("y", "x", "zl", "zh"))
    core = lax.axis_index("core")
    modulus = facet_width * nx * nzh
    uv_cols = modulus // SUB
    periods = rows_local // STRIP
    rows_each = STRIP // (nzl * ny * nx)
    count = subgrid_offsets.shape[1]
    strips = strip_offsets.shape[0]
    blocks = facet_width // SUB
    vmem = pl.BlockSpec(memory_space=VMEM)
    half = jax.ShapeDtypeStruct((2 * STRIP, facet_width), BF16)

    hbm = pl.BlockSpec(memory_space=pltpu.HBM)

    swap = [(0, 1), (1, 0)]
    received = lax.ppermute(model_image, "core", swap)

    lines = rows_each * count
    order = np.arange(uv_cols).reshape(nzh, nx, blocks).transpose(0, 2, 1).reshape(-1)
    block = block_tables(order, uv_cols, rows_each)
    square = jax.ShapeDtypeStruct((2 * STRIP, 2 * STRIP), BF16)
    turned = jax.ShapeDtypeStruct((count, SUB), F32)
    grid = jax.ShapeDtypeStruct((weight_grids.shape[0], 16, SUB), BF16)
    sources = (
        model_image, row_table(rows_each), block, weight_grids,
        strip_offsets, subgrid_offsets, grid_index,
    )
    folded, phases, spread, weights, other, cos_d, sin_d = pl.pallas_call(
        functools.partial(prepare_kernel, modulus, rows_each),
        out_shape=(
            half,
            square,
            jax.ShapeDtypeStruct((2 * lines, block.shape[2]), BF16),
            jax.ShapeDtypeStruct((lines, SUB), F32),
            jax.ShapeDtypeStruct((8, 256), F32),
            turned,
            turned,
        ),
        in_specs=[hbm] * len(sources),
        out_specs=(vmem,) * 7,
        scratch_shapes=[VMEM(a.shape, a.dtype) for a in (model_image, square, block, grid)]
        + [
            SMEM(strip_offsets.shape, I32),
            VMEM(subgrid_offsets.shape, I32),
            VMEM(grid_index.shape, I32),
            pltpu.SemaphoreType.DMA((16,)),
        ],
        cost_estimate=pl.CostEstimate(flops=8 * MIB, bytes_accessed=4 * MIB, transcendentals=0),
        compiler_params=grant(12),
        name="prepare",
    )(*(pltpu.with_memory_space_constraint(a, pltpu.HBM) for a in sources))
    partial = pl.pallas_call(
        row_kernel,
        out_shape=half,
        in_specs=[vmem] * 4,
        out_specs=vmem,
        compiler_params=grant(8),
        name="row_transform",
    )(other, phases, folded, received)
    fourier = column_table()
    zl, y = (lax.axis_index(a) for a in ("zl", "y"))
    first = ((zl * ny + y) * GRID["core"] + core) * rows_local
    cos_x, sin_x = turn(
        strip_offsets[:, None] * (first + jnp.arange(rows_local, dtype=I32)[None]), modulus
    )
    partial, fourier = lax.optimization_barrier((partial, fourier))

    parts = exchange(partial.reshape(ny, -1, facet_width), FIRST)
    share = pl.pallas_call(
        sum_kernel,
        out_shape=jax.ShapeDtypeStruct(parts.shape[1:], BF16),
        in_specs=[vmem],
        out_specs=vmem,
        compiler_params=grant(4),
        name="row_sum",
    )(parts)
    parts = exchange(share.reshape(nzl * nx, 2 * rows_each, facet_width), SECOND)
    parts = parts.reshape(nx, nzl, 2 * rows_each, facet_width)
    strip = jnp.sum(parts.astype(F32), axis=1).astype(BF16).reshape(-1, facet_width)
    whole = lax.all_gather(strip, "zh", axis=0, tiled=True)

    back = pl.pallas_call(
        functools.partial(middle_kernel, lines),
        out_shape=jax.ShapeDtypeStruct((nx * 2 * rows_each, facet_width), BF16),
        in_specs=[vmem] * 6,
        out_specs=vmem,
        compiler_params=grant(16),
        name="subgrids",
    )(spread, cos_d, sin_d, weights, fourier, whole)

    back = back.reshape(nx, 1, 2 * rows_each, facet_width)
    back = jnp.broadcast_to(back, (nx, nzl, *back.shape[2:]))
    back = back.reshape(nx * nzl, 2 * rows_each, facet_width)
    back = exchange(back, SECOND).reshape(1, -1, facet_width)
    back = jnp.broadcast_to(back, (ny, *back.shape[1:]))
    image = exchange(back, FIRST).reshape(2 * STRIP, facet_width)

    scale = 1.0 / (modulus * math.sqrt(count * SUB) * math.sqrt(strips * STRIP))
    received = lax.ppermute(image, "core", swap)
    full = jax.ShapeDtypeStruct((rows_local, facet_width), F32)
    own, other_phases = pl.pallas_call(
        own_kernel,
        out_shape=(full, square),
        in_specs=[vmem] * 4,
        out_specs=(vmem, vmem),
        scratch_shapes=[VMEM(square.shape, BF16)],
        cost_estimate=pl.CostEstimate(flops=512 * MIB, bytes_accessed=MIB, transcendentals=0),
        compiler_params=grant(8),
        name="own_part",
    )(return_table(rows_each), cos_x, sin_x, image)
    return pl.pallas_call(
        functools.partial(update_kernel, scale),
        out_shape=full,
        in_specs=[vmem] * 3,
        out_specs=hbm,
        scratch_shapes=[VMEM(full.shape, F32), pltpu.SemaphoreType.DMA((8,))],
        compiler_params=grant(8),
        name="update",
    )(other_phases, own, received)


def solution(mesh):
    finer = Mesh(mesh.devices.reshape(tuple(GRID.values())), tuple(GRID))
    rows, cols = ("zl", "y", "core"), ("zh", "x")
    return jax.shard_map(
        body,
        mesh=finer,
        in_specs=(P(rows, cols), P(), P(), P(), P()),
        out_specs=P(rows, cols),
        check_vma=False,
    )
```

```python
import functools
import math

import jax
import jax.numpy as jnp
import ml_dtypes
import numpy as np
from jax import lax
from jax.experimental import pallas as pl
from jax.experimental.pallas import tpu as pltpu
from jax.sharding import Mesh
from jax.sharding import PartitionSpec as P

F32 = jnp.float32
BF16 = jnp.bfloat16
I32 = jnp.int32
STRIP = 256
SUB = 256
GRID = {"zl": 4, "y": 4, "core": 2, "zh": 4, "x": 4}
FIRST = ("zl", "y", "core")
SECOND = ("zl", "y", "core", "x")
VMEM = pltpu.VMEM
SMEM = pltpu.SMEM
MIB = 1 << 20


def grant(mib):
    return pltpu.CompilerParams(vmem_limit_bytes=mib * MIB)


def groups(axes):
    place = np.arange(math.prod(GRID[a] for a in axes)).reshape([GRID[a] for a in axes])
    lists = []
    for core in range(GRID["core"]):
        along_y = (core == 0) == (axes == FIRST)
        part = place[:, :, core] if along_y else place[:, :, core].swapaxes(0, 1)
        lists += [row.T.reshape(-1).tolist() for row in part]
    return lists


def exchange(value, axes):
    return lax.all_to_all(value, axes, 0, 0, axis_index_groups=groups(axes), tiled=True)


def turn(numerator, denominator):
    angle = (numerator % denominator).astype(F32) * (2.0 * math.pi / denominator)
    return jnp.cos(angle), jnp.sin(angle)


def fixed(values):
    return jnp.asarray(np.asarray(values, dtype=ml_dtypes.bfloat16))


def row_table(rows_each):
    r = np.arange(STRIP).reshape(-1, 1, rows_each, 1, 1)
    p = np.arange(2).reshape(1, 2, 1, 1, 1)
    q = np.arange(2).reshape(1, 1, 1, 2, 1)
    b = np.arange(STRIP).reshape(1, 1, 1, 1, -1)
    phase = 2.0 * np.pi * ((r * b) % STRIP) / STRIP + (p - q) * (np.pi / 2)
    return fixed(np.cos(phase.reshape(2 * STRIP, 2 * STRIP)))


def return_table(rows_each):
    b = np.arange(STRIP).reshape(-1, 1, 1, 1)
    r = np.arange(STRIP).reshape(1, -1, 1, rows_each)
    p = np.arange(2).reshape(1, 1, 2, 1)
    phase = (2.0 * np.pi * ((r * b) % STRIP) / STRIP + p * (np.pi / 2)).reshape(STRIP, 2 * STRIP)
    return fixed(np.concatenate([np.cos(phase), -np.sin(phase)], axis=0))


def column_table():
    d = np.arange(SUB)
    phase = 2.0 * np.pi * (np.outer(d, d) % SUB) / SUB
    cos, sin = np.cos(phase), np.sin(phase)
    return fixed(np.block([[cos, -sin], [sin, cos]]))


def block_tables(order, uv_cols, rows_each):
    u = np.arange(uv_cols).reshape(1, -1, 1, 1, 1, 1)
    p = np.arange(2).reshape(2, 1, 1, 1, 1, 1)
    c = order.reshape(1, 1, -1, 1, 1, 1)
    q = np.arange(2).reshape(1, 1, 1, 2, 1, 1)
    phase = 2.0 * np.pi * ((u * c) % uv_cols) / uv_cols + (p - q) * (np.pi / 2)
    table = np.broadcast_to(np.cos(phase), (2, uv_cols, order.size, 2, rows_each, 1))
    return fixed(table.reshape(2, uv_cols, -1))


def coefficients(strip, rows_of, periods, uv_cols, offset_ref):
    zl, y = (lax.axis_index(a) for a in ("zl", "y"))
    first = ((zl * GRID["y"] + y) * GRID["core"] + rows_of) * periods
    pairs = []
    for a in range(periods):
        place = (offset_ref[strip] * (first + a)) & (uv_cols - 1)
        cos, sin = F32(1.0), F32(0.0)
        for digit in range(uv_cols.bit_length() - 1):
            angle = 2.0 * math.pi * (1 << digit) / uv_cols
            by_cos, by_sin = round(math.cos(angle), 15), round(math.sin(angle), 15)
            on = ((place >> digit) & 1) == 1
            cos, sin = (
                jnp.where(on, cos * by_cos - sin * by_sin, cos),
                jnp.where(on, sin * by_cos + cos * by_sin, sin),
            )
        pairs.append((cos, sin))
    return pairs


def spin(place, modulus):
    cos, sin = jnp.ones(place.shape, F32), jnp.zeros(place.shape, F32)
    for digit in range(modulus.bit_length() - 1):
        angle = 2.0 * math.pi * (1 << digit) / modulus
        by_cos, by_sin = round(math.cos(angle), 15), round(math.sin(angle), 15)
        on = ((place >> digit) & 1) == 1
        cos, sin = (
            jnp.where(on, cos * by_cos - sin * by_sin, cos),
            jnp.where(on, sin * by_cos + cos * by_sin, sin),
        )
    return cos, sin


def one_hot(condition):
    return jnp.where(condition, 1.0, 0.0).astype(BF16)


OVER_ROWS = (((0,), (0,)), ((), ()))


def prepare_kernel(
    modulus, rows_each, image_hbm, row_hbm, block_hbm, grid_hbm, offset_hbm, shift_hbm, chosen_hbm,
    folded_ref, phases_ref, spread_ref, weight_ref, other_ref, cos_ref, sin_ref,
    image_ref, row_ref, block_ref, grid_ref, offset_ref, shift_ref, chosen_ref, sems,
):
    core = lax.axis_index("core")
    here = pl.ds(core, 1)
    tile, pieces = 16, 4
    uv_cols = block_ref.shape[1]
    periods = image_ref.shape[0] // STRIP
    y, zl = lax.axis_index("y"), lax.axis_index("zl")
    early, late = jnp.where(core == 0, y, zl), jnp.where(core == 0, zl, y)
    quad = (early * GRID["x"] + lax.axis_index("x")) * GRID["zl"] + late
    first = rows_each * quad
    base = pl.multiple_of((first // tile) * tile, tile)
    pairs = [
        (offset_hbm, offset_ref),
        (shift_hbm, shift_ref),
        (chosen_hbm, chosen_ref),
        (block_hbm, block_ref),
        (grid_hbm.at[:, pl.ds(base, tile), :], grid_ref),
        (row_hbm, row_ref),
    ]
    ahead = len(pairs)
    rows = STRIP // pieces
    for n in range(pieces):
        for a in range(periods):
            at = pl.ds(a * STRIP + n * rows, rows)
            pairs.append((image_hbm.at[at], image_ref.at[at]))
    copies = [pltpu.make_async_copy(*pair, sems.at[n]) for n, pair in enumerate(pairs)]
    for copy in copies:
        copy.start()

    for copy in copies[:4]:
        copy.wait()
    count = shift_ref.shape[1]
    columns = block_ref.shape[2]
    level = lax.broadcasted_iota(I32, (uv_cols, count), 0)
    pick = one_hot(level == shift_ref[here, :])
    row = lax.broadcasted_iota(I32, (count, columns), 1) & (rows_each - 1)
    for part in range(2):
        lines = lax.dot_general(pick, block_ref[part], OVER_ROWS, preferred_element_type=F32)
        for i in range(rows_each):
            at = (part * rows_each + i) * count
            spread_ref[at : at + count, :] = jnp.where(row == i, lines, 0.0).astype(BF16)
    number = lax.broadcasted_iota(I32, (uv_cols, SUB), 0).astype(F32).astype(BF16)
    shift = lax.dot_general(pick, number, OVER_ROWS, preferred_element_type=F32).astype(I32)
    cos_ref[...], sin_ref[...] = spin(
        shift * lax.broadcasted_iota(I32, shift.shape, 1) & (modulus - 1), modulus
    )
    copies[4].wait()
    grids = grid_ref.shape[0]
    grid_rows = jnp.concatenate([grid_ref[g] for g in range(grids)], axis=0)
    line = lax.broadcasted_iota(I32, (grids * tile, count), 0)
    chosen = chosen_ref[here, :] * tile + (first - base)
    for i in range(rows_each):
        pick = one_hot(line == chosen + i)
        weight_ref[i * count : (i + 1) * count, :] = lax.dot_general(
            pick, grid_rows, OVER_ROWS, preferred_element_type=F32
        )

    copies[5].wait()
    step = 16
    b = lax.broadcasted_iota(I32, (1, STRIP), 1)
    cos, sin = spin(offset_ref[core] * b & (modulus - 1), modulus)
    for at in range(0, row_ref.shape[0], step):
        block = slice(at, at + step)
        left = row_ref[block, :STRIP].astype(F32)
        right = row_ref[block, STRIP:].astype(F32)
        phases_ref[block, :STRIP] = (left * cos - right * sin).astype(BF16)
        phases_ref[block, STRIP:] = (right * cos + left * sin).astype(BF16)

    factors = coefficients(core, 1 - core, periods, uv_cols, offset_ref)
    for n, value in enumerate(value for pair in factors for value in pair):
        other_ref[n : n + 1, :] = jnp.full((1, other_ref.shape[1]), value, F32)
    factors = coefficients(core, core, periods, uv_cols, offset_ref)
    width = 512
    for n in range(pieces):
        for a in range(periods):
            copies[ahead + n * periods + a].wait()
        for at in range(n * rows, (n + 1) * rows, step):
            for lane in range(0, image_ref.shape[1], width):
                lanes = slice(lane, lane + width)
                real = imag = 0.0
                for a, (cos, sin) in enumerate(factors):
                    pixels = image_ref[a * STRIP + at : a * STRIP + at + step, lanes].astype(F32)
                    real = real + pixels * cos
                    imag = imag - pixels * sin
                folded_ref[at : at + step, lanes] = real.astype(BF16)
                folded_ref[STRIP + at : STRIP + at + step, lanes] = imag.astype(BF16)


def row_kernel(other_ref, phases_ref, folded_ref, image_ref, out_ref):
    periods = image_ref.shape[0] // STRIP
    step = other_ref.shape[1]
    pairs = [
        (other_ref[2 * a : 2 * a + 1, :], other_ref[2 * a + 1 : 2 * a + 2, :]) for a in range(periods)
    ]
    for lane in range(0, out_ref.shape[1], step):
        lanes = slice(lane, lane + step)
        pixels = [image_ref[a * STRIP : (a + 1) * STRIP, lanes].astype(F32) for a in range(periods)]
        real = folded_ref[:STRIP, lanes].astype(F32)
        imag = folded_ref[STRIP:, lanes].astype(F32)
        for value, (cos, sin) in zip(pixels, pairs):
            real = real + value * cos
            imag = imag - value * sin
        total = jnp.concatenate([real.astype(BF16), imag.astype(BF16)], axis=0)
        out_ref[:, lanes] = jnp.dot(phases_ref[...], total, preferred_element_type=F32).astype(BF16)


def sum_kernel(parts_ref, out_ref):
    step, width = 16, 512
    for at in range(0, out_ref.shape[0], step):
        for lane in range(0, out_ref.shape[1], width):
            here = (slice(at, at + step), slice(lane, lane + width))
            total = parts_ref[(0, *here)].astype(F32)
            for n in range(1, parts_ref.shape[0]):
                total = total + parts_ref[(n, *here)].astype(F32)
            out_ref[here] = total.astype(BF16)


def middle_kernel(lines, spread_ref, cos_ref, sin_ref, weight_ref, fourier_ref, strip_ref, out_ref):
    nzh = GRID["zh"]
    held = strip_ref.shape[0] // nzh
    blocks = strip_ref.shape[1] // SUB
    pieces = [
        strip_ref[z * held : (z + 1) * held, c * SUB : (c + 1) * SUB]
        for z in range(nzh)
        for c in range(blocks)
    ]
    whole = jnp.concatenate(pieces, axis=0)
    mixed = jnp.dot(spread_ref[...], whole, preferred_element_type=F32)
    repeat = lines // cos_ref.shape[0]
    cos = jnp.concatenate([cos_ref[...]] * repeat, axis=0)
    sin = jnp.concatenate([sin_ref[...]] * repeat, axis=0)
    real, imag = mixed[:lines], mixed[lines:]
    turned = jnp.concatenate([real * cos + imag * sin, imag * cos - real * sin], axis=1)
    spectra = jnp.dot(turned.astype(BF16), fourier_ref[...], preferred_element_type=F32)
    weight = weight_ref[...]
    weighted = jnp.concatenate([spectra[:, :SUB] * weight, -spectra[:, SUB:] * weight], axis=1)
    returned = jnp.dot(weighted.astype(BF16), fourier_ref[...], preferred_element_type=F32)
    real, imag = returned[:, :SUB], -returned[:, SUB:]
    turned = jnp.concatenate([real * cos - imag * sin, imag * cos + real * sin], axis=0)
    inside = held * blocks
    mine = spread_ref[:, pl.ds(pl.multiple_of(lax.axis_index("zh") * inside, inside), inside)]
    back = lax.dot_general(
        mine, turned.astype(BF16), (((0,), (0,)), ((), ())), preferred_element_type=F32
    ).astype(BF16)
    for c in range(blocks):
        out_ref[:, c * SUB : (c + 1) * SUB] = back[c * held : (c + 1) * held]


def own_kernel(scale, return_ref, cos_ref, sin_ref, image_ref, out_ref, other_ref, own_ref):
    core = lax.axis_index("core")
    step = 16

    def phases(strip, ref):
        turns = jnp.concatenate(
            [cos_ref[pl.ds(strip, 1), :], sin_ref[pl.ds(strip, 1), :]] * 4, axis=0
        )
        turns = jnp.transpose(turns * scale)
        for at in range(0, turns.shape[0], step):
            b = at % STRIP
            cos, sin = turns[at : at + step, 0:1], turns[at : at + step, 1:2]
            ref[at : at + step, :] = (
                return_ref[b : b + step, :].astype(F32) * cos
                + return_ref[STRIP + b : STRIP + b + step, :].astype(F32) * sin
            ).astype(BF16)

    phases(core, own_ref)
    for lane in range(0, out_ref.shape[1], 256):
        lanes = slice(lane, lane + 256)
        out_ref[:, lanes] = jnp.dot(own_ref[...], image_ref[:, lanes], preferred_element_type=F32)
    phases(1 - core, other_ref)


def update_kernel(back_ref, own_ref, image_ref, out_hbm, held_ref, sems):
    step = 256
    copies = []
    for lane in range(0, held_ref.shape[1], step):
        lanes = slice(lane, lane + step)
        other = jnp.dot(back_ref[...], image_ref[:, lanes], preferred_element_type=F32)
        held_ref[:, lanes] = own_ref[:, lanes] + other
        for row in range(0, held_ref.shape[0], 128):
            at = (pl.ds(row, 128), pl.ds(lane, step))
            copies.append(
                pltpu.make_async_copy(held_ref.at[at], out_hbm.at[at], sems.at[len(copies)])
            )
            copies[-1].start()
    for copy in copies:
        copy.wait()


def body(model_image, weight_grids, strip_offsets, subgrid_offsets, grid_index):
    rows_local, facet_width = model_image.shape
    ny, nx, nzl, nzh = (GRID[a] for a in ("y", "x", "zl", "zh"))
    core = lax.axis_index("core")
    modulus = facet_width * nx * nzh
    uv_cols = modulus // SUB
    periods = rows_local // STRIP
    rows_each = STRIP // (nzl * ny * nx)
    count = subgrid_offsets.shape[1]
    strips = strip_offsets.shape[0]
    blocks = facet_width // SUB
    vmem = pl.BlockSpec(memory_space=VMEM)
    half = jax.ShapeDtypeStruct((2 * STRIP, facet_width), BF16)

    hbm = pl.BlockSpec(memory_space=pltpu.HBM)

    swap = [(0, 1), (1, 0)]
    received = lax.ppermute(model_image, "core", swap)

    lines = rows_each * count
    order = np.arange(uv_cols).reshape(nzh, nx, blocks).transpose(0, 2, 1).reshape(-1)
    block = block_tables(order, uv_cols, rows_each)
    square = jax.ShapeDtypeStruct((2 * STRIP, 2 * STRIP), BF16)
    turned = jax.ShapeDtypeStruct((count, SUB), F32)
    grid = jax.ShapeDtypeStruct((weight_grids.shape[0], 16, SUB), BF16)
    sources = (
        model_image, row_table(rows_each), block, weight_grids,
        strip_offsets, subgrid_offsets, grid_index,
    )
    folded, phases, spread, weights, other, cos_d, sin_d = pl.pallas_call(
        functools.partial(prepare_kernel, modulus, rows_each),
        out_shape=(
            half,
            square,
            jax.ShapeDtypeStruct((2 * lines, block.shape[2]), BF16),
            jax.ShapeDtypeStruct((lines, SUB), F32),
            jax.ShapeDtypeStruct((8, 256), F32),
            turned,
            turned,
        ),
        in_specs=[hbm] * len(sources),
        out_specs=(vmem,) * 7,
        scratch_shapes=[VMEM(a.shape, a.dtype) for a in (model_image, square, block, grid)]
        + [
            SMEM(strip_offsets.shape, I32),
            VMEM(subgrid_offsets.shape, I32),
            VMEM(grid_index.shape, I32),
            pltpu.SemaphoreType.DMA((16,)),
        ],
        cost_estimate=pl.CostEstimate(flops=8 * MIB, bytes_accessed=4 * MIB, transcendentals=0),
        compiler_params=grant(12),
        name="prepare",
    )(*(pltpu.with_memory_space_constraint(a, pltpu.HBM) for a in sources))
    partial = pl.pallas_call(
        row_kernel,
        out_shape=half,
        in_specs=[vmem] * 4,
        out_specs=vmem,
        compiler_params=grant(8),
        name="row_transform",
    )(other, phases, folded, received)
    fourier = column_table()
    zl, y = (lax.axis_index(a) for a in ("zl", "y"))
    first = ((zl * ny + y) * GRID["core"] + core) * rows_local
    cos_x, sin_x = turn(
        strip_offsets[:, None] * (first + jnp.arange(rows_local, dtype=I32)[None]), modulus
    )
    partial, fourier = lax.optimization_barrier((partial, fourier))

    parts = exchange(partial.reshape(ny, -1, facet_width), FIRST)
    share = pl.pallas_call(
        sum_kernel,
        out_shape=jax.ShapeDtypeStruct(parts.shape[1:], BF16),
        in_specs=[vmem],
        out_specs=vmem,
        compiler_params=grant(4),
        name="row_sum",
    )(parts)
    parts = exchange(share.reshape(nzl * nx, 2 * rows_each, facet_width), SECOND)
    parts = parts.reshape(nx, nzl, 2 * rows_each, facet_width)
    strip = jnp.sum(parts.astype(F32), axis=1).astype(BF16).reshape(-1, facet_width)
    whole = lax.all_gather(strip, "zh", axis=0, tiled=True)

    back = pl.pallas_call(
        functools.partial(middle_kernel, lines),
        out_shape=jax.ShapeDtypeStruct((nx * 2 * rows_each, facet_width), BF16),
        in_specs=[vmem] * 6,
        out_specs=vmem,
        compiler_params=grant(16),
        name="subgrids",
    )(spread, cos_d, sin_d, weights, fourier, whole)

    back = back.reshape(nx, 1, 2 * rows_each, facet_width)
    back = jnp.broadcast_to(back, (nx, nzl, *back.shape[2:]))
    back = back.reshape(nx * nzl, 2 * rows_each, facet_width)
    back = exchange(back, SECOND).reshape(1, -1, facet_width)
    back = jnp.broadcast_to(back, (ny, *back.shape[1:]))
    image = exchange(back, FIRST).reshape(2 * STRIP, facet_width)

    scale = 1.0 / (modulus * math.sqrt(count * SUB) * math.sqrt(strips * STRIP))
    received = lax.ppermute(image, "core", swap)
    full = jax.ShapeDtypeStruct((rows_local, facet_width), F32)
    own, other_phases = pl.pallas_call(
        functools.partial(own_kernel, scale),
        out_shape=(full, square),
        in_specs=[vmem] * 4,
        out_specs=(vmem, vmem),
        scratch_shapes=[VMEM(square.shape, BF16)],
        cost_estimate=pl.CostEstimate(flops=512 * MIB, bytes_accessed=MIB, transcendentals=0),
        compiler_params=grant(8),
        name="own_part",
    )(return_table(rows_each), cos_x, sin_x, image)
    return pl.pallas_call(
        update_kernel,
        out_shape=full,
        in_specs=[vmem] * 3,
        out_specs=hbm,
        scratch_shapes=[VMEM(full.shape, F32), pltpu.SemaphoreType.DMA((16,))],
        compiler_params=grant(8),
        name="update",
    )(other_phases, own, received)


def solution(mesh):
    finer = Mesh(mesh.devices.reshape(tuple(GRID.values())), tuple(GRID))
    rows, cols = ("zl", "y", "core"), ("zh", "x")
    return jax.shard_map(
        body,
        mesh=finer,
        in_specs=(P(rows, cols), P(), P(), P(), P()),
        out_specs=P(rows, cols),
        check_vma=False,
    )
```
